32 devices in a mesh: grp: 4 (over x, core), dev: 8 (over z, y).
Axes of the slice: x: 2, y: 2, z: 4, core: 2. Of those that a mesh axis runs over, the one named last changes fastest.
Arguments:
- energies: bfloat16 [4096, 32768], P(('grp', 'dev')), may hold values from -48 to 48
- triples: int32 [4096, 3], P(('grp', 'dev')), may hold values from 0 to 113, as said below
- pair_surfaces: float32 [7200, 1024], P('dev'), may hold values from -24 to 24
- pair_slot: int32 [114, 114], replicated, may hold values from 0 to 7199, as said below
- single_surfaces: float32 [120, 32], P('dev'), may hold values from -12 to 12
- modals: float32 [120, 512], P('dev'), may hold values from -1 to 1
- mode_slot: int32 [114], replicated, may hold values from 0 to 119, as said below
Outputs:
- coefficients: bfloat16 [4096, 4096], P(('grp', 'dev'))
- triple_energy: float32 [4096], P(('grp', 'dev'))
- mean_field: float32 [120, 256], P('dev')
The draws below stay inside these ranges and needn't reach their ends.
Inputs may be any that keep to these rules, and one draw needn't show every extreme that they name: The three modes of a row are distinct. Rows come in blocks of 128, one block to each device in the order of the triples' placement; all rows of a block share their first mode m, and m * (number of groups along grp) // 114 is the block's index along grp. Counting one need for each row and each of its three pairs, the rows of one block need exactly 48 surfaces from each owner along dev, the owner of pair_slot row q being q // 900. `pair_slot`: Symmetric; for two distinct modes it names the row of pair_surfaces that holds their surface, distinct pairs naming distinct rows; the diagonal is 0. `mode_slot`: distinct modes name distinct rows.
All inputs are finite; a program needn't handle non-finite values.
Results may differ from the reference program's by a relative error of at most 0.001.
Values sent between devices are 32-bit elements; how exact they have to be, the bound alone decides.
A program may use at most 128 MiB of HBM per device.

```python
import jax
import jax.numpy as jnp
from jax import lax

M = 114
G = 32
KEEP = 16
S = 16
TRI_DEV = 128
TRIPLES = 4096
MODE_DEV = 15
MODE_SLOTS = 120
PAIR_DEV = 900
PAIR_SLOTS = 7200
N_GRP = 4
N_DEV = 8


def mode_layout(key):
    mode_order = jax.random.permutation(jax.random.fold_in(key, 11), M).astype(jnp.int32)
    ranking = jnp.zeros((M,), jnp.int32).at[mode_order].set(jnp.arange(M, dtype=jnp.int32))
    return (mode_order, ranking)


def draw_mode_slot(key, part):
    mode_order, ranking = mode_layout(key)
    return ranking % N_DEV * MODE_DEV + ranking // N_DEV


def draw_pair_slot(key, part):
    mode_order, ranking = mode_layout(key)
    owner_of = ranking % N_DEV
    cell_count = M * M
    mode_ids = jnp.arange(M, dtype=jnp.int32)
    above = mode_ids[:, None] < mode_ids[None, :]
    pair_owner = (owner_of[:, None] + owner_of[None, :]) % N_DEV
    priority = jax.random.permutation(jax.random.fold_in(key, 23), cell_count).astype(jnp.int32).reshape(M, M)
    sort_keys = jnp.where(above, pair_owner * cell_count + priority, N_DEV * cell_count + priority).reshape(cell_count)
    sorted_cells = jnp.argsort(sort_keys)
    position = jnp.zeros((cell_count,), jnp.int32).at[sorted_cells].set(jnp.arange(cell_count, dtype=jnp.int32))
    flat_owner = pair_owner.reshape(cell_count)
    flat_above = above.reshape(cell_count)
    owner_ids = jnp.arange(N_DEV, dtype=jnp.int32)
    per_owner = jnp.sum(((flat_owner[:, None] == owner_ids[None, :]) & flat_above[:, None]).astype(jnp.int32), axis=0)
    starts = jnp.cumsum(per_owner) - per_owner
    slot_ids = flat_owner * PAIR_DEV + position - starts[flat_owner]
    slot_table = jnp.where(flat_above, slot_ids, 0).reshape(M, M)
    return slot_table + slot_table.T


def pick_member(member_key, classes, avoid_first, avoid_second, mode_order):
    places = jnp.arange(MODE_DEV, dtype=jnp.int32)
    rank_grid = classes[:, None] + places[None, :] * N_DEV
    members = mode_order[jnp.minimum(rank_grid, M - 1)]
    usable = (rank_grid < M) & (members != avoid_first[:, None]) & (members != avoid_second[:, None])
    scores = jax.random.randint(member_key, rank_grid.shape, 0, 1 << 20) * MODE_DEV + places[None, :]
    scores = jnp.where(usable, scores, -1)
    chosen = jnp.argmax(scores, axis=1)
    return jnp.take_along_axis(members, chosen[:, None], axis=1)[:, 0]


def draw_triples(key, part):
    mode_order, ranking = mode_layout(key)

    def one_block(block_index):
        block_key = jax.random.fold_in(jax.random.fold_in(key, 37), block_index)
        group_id = block_index // N_DEV
        lowest = (group_id * M + N_GRP - 1) // N_GRP
        beyond = ((group_id + 1) * M + N_GRP - 1) // N_GRP
        leading = lowest + jax.random.randint(jax.random.fold_in(block_key, 1), (), 0, 1 << 20) % (beyond - lowest)
        row_ids = jnp.arange(TRI_DEV, dtype=jnp.int32)
        class_second = row_ids % N_DEV
        class_third = (class_second + row_ids // N_DEV % N_DEV) % N_DEV
        lead_column = jnp.zeros((TRI_DEV,), jnp.int32) + leading
        second = pick_member(jax.random.fold_in(block_key, 2), class_second, lead_column, lead_column, mode_order)
        third_mode = pick_member(jax.random.fold_in(block_key, 3), class_third, lead_column, second, mode_order)
        return jnp.stack([lead_column, second, third_mode], axis=1).astype(jnp.int32)
    blocks = jax.vmap(one_block)(jnp.arange(N_GRP * N_DEV, dtype=jnp.int32))
    return blocks.reshape(TRIPLES, 3)


def shard_levels(key, shape, shards, smallest, high):
    factor_of, own = 1.0, jax.random.fold_in(key, 6)
    for axis_at, blocks in shards:
        steps = jnp.exp(jax.random.uniform(jax.random.fold_in(own, axis_at), (blocks,), jnp.float32, smallest / len(shards), high / len(shards)))
        factor_of = factor_of * jnp.repeat(steps, shape[axis_at] // blocks).reshape([-1 if axis == axis_at else 1 for axis in range(len(shape))])
    return factor_of


def gaussian(rng, extent, deviation, bound, shards=(), kind=jnp.bfloat16):
    array = jax.random.normal(rng, extent, jnp.float32) * deviation
    if len(shards) > 0:
        array = shard_levels(rng, extent, shards, -0.22, 0.18) * array
    return jnp.clip(array, min=-bound, max=bound).astype(kind)


def setup_inputs(seed: int = 0) -> dict:
    key_list = jax.random.split(jax.random.key(seed), 8)
    energies = gaussian(key_list[0], (TRIPLES, G * G * G), 8.0, 48.0, ((0, 32),))
    triples = draw_triples(jax.random.fold_in(key_list[7], 71), 0)
    pair_surfaces = gaussian(key_list[2], (PAIR_SLOTS, G * G), 4.0, 24.0, ((0, 8),), jnp.float32)
    pair_slot = draw_pair_slot(jax.random.fold_in(key_list[7], 71), 0)
    single_surfaces = gaussian(key_list[4], (MODE_SLOTS, G), 2.0, 12.0, ((0, 8),), jnp.float32)
    modals = gaussian(key_list[5], (MODE_SLOTS, G * S), G ** -0.5, 1.0, ((0, 8),), jnp.float32)
    mode_slot = draw_mode_slot(jax.random.fold_in(key_list[7], 71), 0)
    return dict(energies=energies, triples=triples, pair_surfaces=pair_surfaces, pair_slot=pair_slot, single_surfaces=single_surfaces, modals=modals, mode_slot=mode_slot)


highest = lax.Precision.HIGHEST


def tables():
    orders = jnp.arange(KEEP, dtype=jnp.float32)
    points = jnp.arange(G, dtype=jnp.float32) + 0.5
    cosines = jnp.cos(jnp.pi * orders[:, None] * points[None, :] / G)
    weights = jnp.where(orders == 0, 1.0, 2.0) / G
    return cosines, weights[:, None] * cosines


def chebyshev_fit(values, fitter):
    number = values.shape[0]
    section_one = jnp.einsum('cg,bgx->bcx', fitter, values.reshape(number, G, G * G), precision=highest)
    section_one = section_one.reshape(number, KEEP, G, G)
    section_two = jnp.einsum('dh,bchl->bcdl', fitter, section_one, precision=highest)
    return jnp.einsum('el,bcdl->bcde', fitter, section_two, precision=highest)


def oriented(picked, lower_ends, upper_ends, width):
    square = picked.reshape(-1, width, width)
    return jnp.where((lower_ends < upper_ends)[:, None, None], square, jnp.swapaxes(square, 1, 2))


def reference(energies, triples, pair_surfaces, pair_slot, single_surfaces, modals, mode_slot):
    cosines, fitter = tables()
    shaped = modals.reshape(MODE_SLOTS, G, S)
    ground = jnp.einsum('mg,cg->mc', shaped[:, :, 0] ** 2, cosines, precision=highest)
    blocks = TRIPLES // TRI_DEV
    slot_range = jnp.arange(MODE_SLOTS, dtype=jnp.int32)

    def advance(totals, inputs):
        energy, mode_rows = inputs
        lead_mode = mode_rows[:, 0]
        second = mode_rows[:, 1]
        third_mode = mode_rows[:, 2]
        pair_first = oriented(pair_surfaces[pair_slot[lead_mode, second]], lead_mode, second, G)
        pair_second = oriented(pair_surfaces[pair_slot[lead_mode, third_mode]], lead_mode, third_mode, G)
        pair_third = oriented(pair_surfaces[pair_slot[second, third_mode]], second, third_mode, G)
        slot_first = mode_slot[lead_mode]
        slot_second = mode_slot[second]
        slot_third = mode_slot[third_mode]
        single_first = single_surfaces[slot_first]
        single_second = single_surfaces[slot_second]
        single_third = single_surfaces[slot_third]
        values = (energy.astype(jnp.float32).reshape(-1, G, G, G)
                  - pair_first[:, :, :, None] - pair_second[:, :, None, :] - pair_third[:, None, :, :]
                  - single_first[:, :, None, None] - single_second[:, None, :, None] - single_third[:, None, None, :])
        fitted = chebyshev_fit(values, fitter)
        ground_first = ground[slot_first]
        ground_second = ground[slot_second]
        ground_third = ground[slot_third]
        field_first = jnp.einsum('bcde,bd,be->bc', fitted, ground_second, ground_third, precision=highest)
        field_second = jnp.einsum('bcde,bc,be->bd', fitted, ground_first, ground_third, precision=highest)
        field_third = jnp.einsum('bcde,bc,bd->be', fitted, ground_first, ground_second, precision=highest)
        energy_out = jnp.sum(field_first * ground_first, axis=1)
        slot_ids = jnp.concatenate([slot_first, slot_second, slot_third])
        onehot = (slot_range[:, None] == slot_ids[None, :]).astype(jnp.float32)
        fields = jnp.concatenate([field_first, field_second, field_third], axis=0)
        totals = totals + jnp.dot(onehot, fields, precision=highest)
        return totals, (fitted.reshape(-1, KEEP * KEEP * KEEP).astype(jnp.bfloat16), energy_out)

    moments, (coefficients, triple_energy) = lax.scan(
        advance, jnp.zeros((MODE_SLOTS, KEEP), jnp.float32),
        (energies.reshape(blocks, TRI_DEV, G * G * G), triples.reshape(blocks, TRI_DEV, 3)))
    weighted = jnp.dot(moments, cosines, precision=highest)
    mean_field = jnp.einsum('mga,mg,mgb->mab', shaped, weighted, shaped, precision=highest).reshape(MODE_SLOTS, S * S)
    return coefficients.reshape(TRIPLES, KEEP * KEEP * KEEP), triple_energy.reshape(TRIPLES), mean_field
```

```python
import functools

import jax
import jax.numpy as jnp
import numpy as np
from jax import lax
from jax.experimental import pallas as pl
from jax.experimental.pallas import tpu as pltpu
from jax.sharding import PartitionSpec as P

G = 32
KEEP = 16
S = 16
AREA = KEEP * KEEP
HALF = G // 2
LANES = 128
FITS = 4
CHUNKS = 8
MESH = pl.DeviceIdType.MESH
f32 = jnp.float32
bf16 = jnp.bfloat16
highest = lax.Precision.HIGHEST


def np_tables():
    orders = np.arange(KEEP, dtype=np.float64)
    points = np.arange(G, dtype=np.float64) + 0.5
    cosines = np.cos(np.pi * orders[:, None] * points[None, :] / G)
    weights = np.where(orders == 0, 1.0, 2.0) / G
    return cosines, weights[:, None] * cosines


COS, FIT = np_tables()


def split_np(values):
    values = np.asarray(values, np.float32)
    high = values.astype(jnp.bfloat16)
    return high, (values - high.astype(np.float32)).astype(jnp.bfloat16)


INNER = np.einsum("dh,el->dehl", FIT, FIT).reshape(AREA, G * G)
WEIGHTS = np.concatenate(split_np(INNER), axis=0)
SMALL = np.concatenate([np.repeat(COS, S, axis=1), FIT, np.zeros((KEEP, LANES - G))], axis=1).astype(np.float32)


def round_up(value, step):
    return -(-value // step) * step


def iota(shape, axis):
    return lax.broadcasted_iota(jnp.int32, shape, axis)


def nn(a, b, precision=None):
    return lax.dot_general(a, b, (((1,), (0,)), ((), ())), precision=precision, preferred_element_type=f32)


def nt(a, b, precision=None):
    return lax.dot_general(a, b, (((1,), (1,)), ((), ())), precision=precision, preferred_element_type=f32)


def tn(a, b, precision=None):
    return lax.dot_general(a, b, (((0,), (0,)), ((), ())), precision=precision, preferred_element_type=f32)


def split(values):
    high = values.astype(bf16)
    return high, (values - high.astype(f32)).astype(bf16)


def ones_at(mask):
    return jnp.where(mask, 1.0, 0.0).astype(bf16)


def total(values, axis):
    return jnp.sum(values, axis=axis, keepdims=True)


def fit_orders(s, d):
    u = [s[j] + s[15 - j] for j in range(8)]
    v = [s[j] - s[15 - j] for j in range(8)]
    uu = [u[j] + u[7 - j] for j in range(4)]
    uv = [u[j] - u[7 - j] for j in range(4)]
    out = []
    for c in range(KEEP):
        if c % 2:
            terms = d
        elif c % 4:
            terms = v
        elif c % 8:
            terms = uv
        else:
            terms = uu
        acc = float(FIT[c, 0]) * terms[0]
        for j in range(1, len(terms)):
            acc = acc + float(FIT[c, j]) * terms[j]
        out.append(acc)
    return out


def kernel(
    energies, triples, surfaces, pair_slot, singles, modals, mode_slot, weights_hbm, small,
    coefficients, energy_out, mean_out,
    values, surf, weights, planes, acc, table, hits, answers, arrived, pair_t, padded, message, received,
    modes_in, exp_modals, deep, moved, moments,
    load_sem, send_msg, recv_msg, send_ans, recv_ans, send_mom, recv_mom,
    *, devices, groups,
):
    number = triples.shape[0]
    needs = 3 * number
    pair_rows = surfaces.shape[0]
    mode_rows = modals.shape[0]
    modes = pair_slot.shape[0]
    capacity = needs // devices
    cap = answers.shape[1]
    slots = devices * cap
    bands = -(-mode_rows // 8)
    offset = 2 * KEEP * bands
    width = moved.shape[2]
    everyone = devices * groups
    me = lax.axis_index("dev")
    group = lax.axis_index("grp")
    flat = group * devices + me

    loads = [pltpu.make_async_copy(weights_hbm, weights, load_sem.at[0])]
    loads.append(pltpu.make_async_copy(surfaces, surf, load_sem.at[1]))
    part = energies.shape[1] // CHUNKS
    for i in range(CHUNKS):
        span = pl.ds(i * part, part)
        loads.append(pltpu.make_async_copy(energies.at[:, span], values.at[:, span], load_sem.at[2 + i]))
    for load in loads:
        load.start()

    barrier = pltpu.get_barrier_semaphore()

    def greet(k, carry):
        other = lax.rem(flat + k, everyone)
        pl.semaphore_signal(
            barrier, inc=1, device_id=(other // devices, lax.rem(other, devices)), device_id_type=MESH
        )
        return carry

    lax.fori_loop(1, everyone, greet, 0)

    padded[...] = jnp.zeros_like(padded)
    padded[0, :number, 0:3] = triples[...].astype(f32)
    padded[1, 0:modes, 0:modes] = pair_slot[...].astype(f32)
    padded[2, 0:1, 0:modes] = mode_slot[...].astype(f32)
    turned = padded[0].T
    picks = [turned[p : p + 1, :].astype(jnp.int32) for p in range(3)]
    rows = iota((LANES, number), 0)
    on = [rows == pick for pick in picks]
    on_hot = [ones_at(x) for x in on]
    pair_ints = padded[1].astype(jnp.int32)
    first_two = jnp.concatenate(on_hot[:2], axis=1)
    lines = 128.0 * nn((pair_ints >> 7).astype(f32).astype(bf16), first_two)
    lines = lines + nn((pair_ints & 127).astype(f32).astype(bf16), first_two)
    chosen = [
        total(jnp.where(on[1], lines[:, :number], 0.0), 0),
        total(jnp.where(on[2], lines[:, :number], 0.0), 0),
        total(jnp.where(on[2], lines[:, number:], 0.0), 0),
    ]
    flips = [picks[0] > picks[1], picks[0] > picks[2], picks[1] > picks[2]]
    pair_ids = (jnp.concatenate(chosen, axis=1) + 0.5).astype(jnp.int32)
    holders = iota((devices, needs), 0)
    held = (pair_ids >= holders * pair_rows) & (pair_ids < (holders + 1) * pair_rows)
    held_hot = ones_at(held)
    owner = total(jnp.where(held, holders, 0), 0)
    local = pair_ids - owner * pair_rows
    before = ones_at(iota((number, number), 0) < iota((number, number), 1))
    seen = jnp.zeros((devices, 1), f32)
    ranks = []
    for p in range(3):
        block = held_hot[:, p * number : (p + 1) * number]
        mine = held[:, p * number : (p + 1) * number]
        ranks.append(total(jnp.where(mine, nn(block, before) + seen, 0.0), 0))
        seen = seen + total(jnp.where(mine, 1.0, 0.0), 1)
    rank = (jnp.concatenate(ranks, axis=1) + 0.5).astype(jnp.int32)
    place = owner * cap + rank
    at_rank = ones_at(iota((LANES, needs), 0) == rank)
    coarse = jnp.where(held, (local >> 4).astype(f32), 0.0).astype(bf16)
    fine = jnp.where(held, (local & 15).astype(f32), 0.0).astype(bf16)
    requests = 16.0 * nt(coarse, at_rank) + nt(fine, at_rank)

    modes_in[...] = jnp.zeros_like(modes_in)
    modes_in[0:mode_rows, 0 : G * S] = modals[...]
    modes_in[0:mode_rows, G * S : G * S + G] = singles[...]
    every = modes_in[:, 0 : G * S]
    spread = small[:, 0 : G * S]
    lane = iota((KEEP, G * S), 1)
    ground_weights = jnp.where((lane & (S - 1)) == 0, spread, 0.0)
    ground_here = nt(every * every, ground_weights, highest)
    single_here = nt(modes_in[:, G * S : G * S + G], small[:, G * S : G * S + G], highest)
    padded[3, 0 : modes_in.shape[0], 0:KEEP] = ground_here
    padded[3, 0 : modes_in.shape[0], KEEP : 2 * KEEP] = single_here
    base = padded[3, 0:8, :]
    for q in range(1, bands):
        base = base + pltpu.roll(padded[3, 8 * q : 8 * q + 8, :], 2 * KEEP * q, 1)
    asked = pltpu.roll(requests, offset, 1)
    top = iota((8, LANES), 0) == 0
    for p in range(devices):
        message[p] = base + jnp.where(top, asked[p : p + 1, :], 0.0)
    received[me] = message[me]

    pl.semaphore_wait(barrier, everyone - 1)

    def message_copy(peer, slot):
        return pltpu.make_async_remote_copy(
            src_ref=message.at[peer], dst_ref=received.at[slot],
            send_sem=send_msg.at[peer], recv_sem=recv_msg.at[slot],
            device_id=(group, peer), device_id_type=MESH,
        )

    def answer_copy(peer, slot):
        return pltpu.make_async_remote_copy(
            src_ref=answers.at[peer], dst_ref=arrived.at[slot],
            send_sem=send_ans.at[peer], recv_sem=recv_ans.at[slot],
            device_id=(group, peer), device_id_type=MESH,
        )

    def each_peer(action):
        def step(k, carry):
            action(lax.rem(me + k, devices))
            return carry

        lax.fori_loop(1, devices, step, 0)

    each_peer(lambda peer: message_copy(peer, me).start())

    loads[0].wait()
    loads[1].wait()
    w_high = weights[0:AREA, :]
    w_low = weights[AREA : 2 * AREA, :]
    table_rows = table.shape[1]
    done = 0
    while done < table_rows:
        size = min(256, table_rows - done)
        have = min(size, pair_rows - done)
        whole = have // 16 * 16
        pieces = []
        if whole:
            pieces.append(surf[done : done + whole, :])
        if size > whole:
            rest = jnp.zeros((size - whole, G * G), f32)
            if have > whole:
                tail = jnp.concatenate(
                    [surf[done + whole : done + have, :], jnp.zeros((16 - (have - whole), G * G), f32)], axis=0
                )
                pieces.append(tail)
                rest = jnp.zeros((size - whole - 16, G * G), f32)
            if rest.shape[0]:
                pieces.append(None)
        at = done
        for piece in pieces:
            if piece is None:
                table[:, at : done + size, :] = jnp.zeros((2, done + size - at, AREA), bf16)
                continue
            high, low = split(piece)
            fitted = nt(high, w_high) + nt(high, w_low) + nt(low, w_high)
            count = piece.shape[0]
            part_high, part_low = split(fitted)
            table[0, at : at + count, :] = part_high
            table[1, at : at + count, :] = part_low
            at += count
        done += size

    each_peer(lambda peer: message_copy(me, peer).wait_recv())
    wanted = jnp.concatenate([received[p, 0:1, :] for p in range(devices)], axis=0)
    wanted = jnp.concatenate([wanted, jnp.zeros((LANES - devices, LANES), f32)], axis=0)
    wanted = (wanted.T[offset : offset + cap if offset + cap <= LANES else LANES, :] + 0.5).astype(jnp.int32)
    in_table = iota((capacity, table_rows), 1)
    if cap > capacity:
        hits[...] = jnp.zeros_like(hits)
    for p in range(devices):
        hits[p, 0:capacity, :] = ones_at(wanted[0:capacity, p : p + 1] == in_table)
    all_hits = hits[...].reshape(slots, table_rows)
    found = nn(all_hits, table[0]) + nn(all_hits, table[1])
    answers[...] = found.reshape(devices, cap, AREA)
    arrived[me] = answers[me]
    each_peer(lambda peer: answer_copy(peer, me).start())

    modes_hot = jnp.concatenate(on_hot, axis=1)
    slot_ids = (nn(padded[2, 0:8, :].astype(bf16), modes_hot)[0:1, :] + 0.5).astype(jnp.int32)
    homes = iota((devices, needs), 0)
    home = (slot_ids >= homes * mode_rows) & (slot_ids < (homes + 1) * mode_rows)
    home_row = total(jnp.where(home, homes, 0), 0)
    at_home = slot_ids - home_row * mode_rows
    spot = home_row * 8 + (at_home & 7)
    spot_hot = ones_at(iota((devices * 8, needs), 0) == spot)
    tables_high, tables_low = split(received[...].reshape(devices * 8, LANES))
    looked = tn(tables_high, spot_hot) + tn(tables_low, spot_hot)
    band = at_home >> 3
    taken = jnp.where(band == 0, looked[0 : 2 * KEEP], 0.0)
    for q in range(1, bands):
        taken = jnp.where(band == q, looked[2 * KEEP * q : 2 * KEEP * (q + 1)], taken)
    ground = [taken[0:KEEP, p * number : (p + 1) * number] for p in range(3)]
    single = [taken[KEEP : 2 * KEEP, p * number : (p + 1) * number] for p in range(3)]

    for load in loads[2:]:
        load.wait()

    def fit_step(step, carry):
        for i in range(FITS):
            j = step * FITS + i
            front = values[:, pl.ds(pl.multiple_of(j * G * G, G * G), G * G)]
            back = values[:, pl.ds(pl.multiple_of((G - 1 - j) * G * G, G * G), G * G)]
            both = jnp.concatenate([front, back], axis=0)
            plane = nt(weights[0:AREA, :], both) + nt(weights[AREA : 2 * AREA, :], both)
            planes[j] = plane[:, :number] + plane[:, number:]
            planes[HALF + j] = plane[:, :number] - plane[:, number:]
        return carry

    lax.fori_loop(0, HALF // FITS, fit_step, 0)

    def order_step(step, carry):
        span = pl.ds(pl.multiple_of(step * 8, 8), 8)
        sums = [planes[j, span, :] for j in range(HALF)]
        differences = [planes[HALF + j, span, :] for j in range(HALF)]
        for c, value in enumerate(fit_orders(sums, differences)):
            acc[c, span, :] = value
        return carry

    lax.fori_loop(0, AREA // 8, order_step, 0)

    rows16 = modes_in.shape[0]
    for g in range(G):
        exp_modals[g * rows16 : (g + 1) * rows16, 0:S] = modes_in[:, g * S : (g + 1) * S]
    pieces = exp_modals[:, 0:S]
    columns = iota((S, AREA), 1)
    index = iota((S, AREA), 0)
    by_a = jnp.where((columns >> 4) == index, 1.0, 0.0)
    by_b = jnp.where((columns & (S - 1)) == index, 1.0, 0.0)
    products = nn(pieces, by_a, highest) * nn(pieces, by_b, highest)
    tall = jnp.concatenate([spread] * (width // KEEP), axis=0)
    own_row = (iota(tall.shape, 1) & (rows16 - 1)) == (iota(tall.shape, 0) >> 4)
    deep[...] = nn(jnp.where(own_row, tall, 0.0), products, highest)

    each_peer(lambda peer: answer_copy(me, peer).wait_recv())
    place_hot = ones_at(iota((slots, needs), 0) == place)
    arrived_high, arrived_low = split(arrived[...].reshape(slots, AREA))
    ordered = tn(arrived_high, place_hot) + tn(arrived_low, place_hot)
    for p in range(3):
        pair_t[p] = ordered[:, p * number : (p + 1) * number]

    def pair_rows_of(p, c):
        straight = pair_t[p, c * KEEP : (c + 1) * KEEP, :]
        turned_rows = pair_t[p, pl.ds(c, KEEP, stride=KEEP), :]
        return jnp.where(flips[p], turned_rows, straight)

    first_row = iota((KEEP, number), 0) == 0
    for c in range(KEEP):
        along_d = pair_rows_of(0, c)
        along_e = pair_rows_of(1, c) + jnp.where(first_row, single[0][c : c + 1, :], 0.0)
        if c == 0:
            along_d = along_d + single[1]
            along_e = along_e + single[2]
            for d in range(KEEP):
                acc[0, d * KEEP : (d + 1) * KEEP, :] -= pair_rows_of(2, d)
        acc[c, pl.ds(0, KEEP, stride=KEEP), :] -= along_d
        acc[c, 0:KEEP, :] -= along_e

    low3, high3 = ground[2][0:8], ground[2][8:16]
    rows1 = [ground[0][c : c + 1, :] for c in range(KEEP)]
    partial1 = [jnp.zeros((8, number), f32) for _ in range(KEEP)]
    field2 = []
    field3 = [jnp.zeros((8, number), f32) for _ in range(2)]
    for d in range(KEEP):
        row2 = ground[1][d : d + 1, :]
        inner = jnp.zeros((8, number), f32)
        for h, part3 in enumerate((low3, high3)):
            weight = row2 * part3
            mixed = jnp.zeros((8, number), f32)
            for c in range(KEEP):
                value = acc[c, d * KEEP + 8 * h : d * KEEP + 8 * h + 8, :]
                partial1[c] = partial1[c] + value * weight
                mixed = mixed + value * rows1[c]
            inner = inner + mixed * part3
            field3[h] = field3[h] + mixed * row2
        field2.append(total(inner, 0))
    field1 = jnp.concatenate([total(x, 0) for x in partial1], axis=0)
    field2 = jnp.concatenate(field2, axis=0)
    field3 = jnp.concatenate(field3, axis=0)
    energy_out[...] = total(field1 * ground[0], 0)

    fields = jnp.concatenate([field1, field2, field3], axis=1)
    fields = jnp.concatenate([fields] * (width // KEEP), axis=0)
    of_row = (iota((width, needs), 0) >> 4) == at_home
    fields_high, fields_low = split(jnp.where(of_row, fields, 0.0))
    home_hot = ones_at(home)
    sums = nt(home_hot, fields_high) + nt(home_hot, fields_low)
    for p in range(devices):
        moved[p] = sums[p : p + 1, :]
    moments[flat] = moved[me]

    def moment_copy(other, owner_dev, slot):
        return pltpu.make_async_remote_copy(
            src_ref=moved.at[owner_dev], dst_ref=moments.at[slot],
            send_sem=send_mom.at[other], recv_sem=recv_mom.at[slot],
            device_id=(other // devices, lax.rem(other, devices)), device_id_type=MESH,
        )

    def each_other(action):
        def step(k, carry):
            action(lax.rem(flat + k, everyone))
            return carry

        lax.fori_loop(1, everyone, step, 0)

    each_other(lambda other: moment_copy(other, lax.rem(other, devices), flat).start())

    for c in range(KEEP):
        coefficients[:, c * AREA : (c + 1) * AREA] = acc[c].T.astype(bf16)

    each_other(lambda other: moment_copy(flat, me, other).wait_recv())
    summed = moments[0]
    for k in range(1, everyone):
        summed = summed + moments[k]
    chosen_rows = (iota((rows16, width), 1) >> 4) == iota((rows16, width), 0)
    mean = nn(jnp.where(chosen_rows, summed, 0.0), deep[...], highest)
    mean_out[...] = mean[0:mode_rows, :]

    each_peer(lambda peer: message_copy(peer, me).wait_send())
    each_peer(lambda peer: answer_copy(peer, me).wait_send())
    each_other(lambda other: moment_copy(other, lax.rem(other, devices), flat).wait_send())


def body(energies, triples, pair_surfaces, pair_slot, single_surfaces, modals, mode_slot):
    devices = lax.axis_size("dev")
    groups = lax.axis_size("grp")
    number = triples.shape[0]
    pair_rows = pair_surfaces.shape[0]
    mode_rows = modals.shape[0]
    cap = round_up(3 * number // devices, 16)
    table_rows = round_up(pair_rows, 256)
    width = round_up(mode_rows * KEEP, LANES)
    rows16 = 16
    everyone = devices * groups
    vmem = pl.BlockSpec(memory_space=pltpu.VMEM)
    anywhere = pl.BlockSpec(memory_space=pl.ANY)
    coefficients, energy, mean = pl.pallas_call(
        functools.partial(kernel, devices=devices, groups=groups),
        in_specs=[anywhere, vmem, anywhere, vmem, vmem, vmem, vmem, anywhere, vmem],
        out_specs=[vmem, vmem, vmem],
        out_shape=[
            jax.ShapeDtypeStruct((number, KEEP * AREA), bf16),
            jax.ShapeDtypeStruct((1, number), f32),
            jax.ShapeDtypeStruct((mode_rows, S * S), f32),
        ],
        scratch_shapes=[
            pltpu.VMEM(energies.shape, bf16),
            pltpu.VMEM(pair_surfaces.shape, f32),
            pltpu.VMEM(WEIGHTS.shape, bf16),
            pltpu.VMEM((G, AREA, number), f32),
            pltpu.VMEM((KEEP, AREA, number), f32),
            pltpu.VMEM((2, table_rows, AREA), bf16),
            pltpu.VMEM((devices, cap, table_rows), bf16),
            pltpu.VMEM((devices, cap, AREA), f32),
            pltpu.VMEM((devices, cap, AREA), f32),
            pltpu.VMEM((3, AREA, number), f32),
            pltpu.VMEM((4, LANES, LANES), f32),
            pltpu.VMEM((devices, 8, LANES), f32),
            pltpu.VMEM((devices, 8, LANES), f32),
            pltpu.VMEM((rows16, SMALL.shape[1]), f32),
            pltpu.VMEM((G * rows16, LANES), f32),
            pltpu.VMEM((width, AREA), f32),
            pltpu.VMEM((devices, 1, width), f32),
            pltpu.VMEM((everyone, 1, width), f32),
            pltpu.SemaphoreType.DMA((2 + CHUNKS,)),
            pltpu.SemaphoreType.DMA((devices,)),
            pltpu.SemaphoreType.DMA((devices,)),
            pltpu.SemaphoreType.DMA((devices,)),
            pltpu.SemaphoreType.DMA((devices,)),
            pltpu.SemaphoreType.DMA((everyone,)),
            pltpu.SemaphoreType.DMA((everyone,)),
        ],
        compiler_params=pltpu.CompilerParams(
            collective_id=0, has_side_effects=True, vmem_limit_bytes=60 * 1024 * 1024
        ),
    )(
        energies, triples, pair_surfaces, pair_slot, single_surfaces, modals, mode_slot.reshape(1, -1),
        jnp.asarray(WEIGHTS), jnp.asarray(SMALL),
    )
    return coefficients, energy.reshape(number), mean


def solution(mesh):
    in_specs = (
        P(("grp", "dev"), None),
        P(("grp", "dev"), None),
        P("dev", None),
        P(),
        P("dev", None),
        P("dev", None),
        P(),
    )
    out_specs = (P(("grp", "dev"), None), P(("grp", "dev")), P("dev", None))
    return jax.shard_map(body, mesh=mesh, in_specs=in_specs, out_specs=out_specs, check_vma=False)
```

```python
import functools

import jax
import jax.numpy as jnp
import numpy as np
from jax import lax
from jax.experimental import pallas as pl
from jax.experimental.pallas import tpu as pltpu
from jax.sharding import PartitionSpec as P

G = 32
KEEP = 16
S = 16
AREA = KEEP * KEEP
HALF = G // 2
LANES = 128
STEPS = 4
EARLY = 1
CHUNKS = 8
SMALLS = 6
MESH = pl.DeviceIdType.MESH
f32 = jnp.float32
bf16 = jnp.bfloat16
highest = lax.Precision.HIGHEST


def np_tables():
    orders = np.arange(KEEP, dtype=np.float64)
    points = np.arange(G, dtype=np.float64) + 0.5
    cosines = np.cos(np.pi * orders[:, None] * points[None, :] / G)
    weights = np.where(orders == 0, 1.0, 2.0) / G
    return cosines, weights[:, None] * cosines


COS, FIT = np_tables()


def split_np(values):
    values = np.asarray(values, np.float32)
    high = values.astype(jnp.bfloat16)
    return high, (values - high.astype(np.float32)).astype(jnp.bfloat16)


INNER = np.einsum("dh,el->dehl", FIT, FIT).reshape(AREA, G * G)
WEIGHTS = np.concatenate(split_np(INNER), axis=0)
SMALL = np.concatenate([np.repeat(COS, S, axis=1), FIT, np.zeros((KEEP, LANES - G))], axis=1).astype(np.float32)


def round_up(value, step):
    return -(-value // step) * step


def iota(shape, axis):
    return lax.broadcasted_iota(jnp.int32, shape, axis)


def nn(a, b, precision=None):
    return lax.dot_general(a, b, (((1,), (0,)), ((), ())), precision=precision, preferred_element_type=f32)


def nt(a, b, precision=None):
    return lax.dot_general(a, b, (((1,), (1,)), ((), ())), precision=precision, preferred_element_type=f32)


def tn(a, b, precision=None):
    return lax.dot_general(a, b, (((0,), (0,)), ((), ())), precision=precision, preferred_element_type=f32)


def split(values):
    high = values.astype(bf16)
    return high, (values - high.astype(f32)).astype(bf16)


def ones_at(mask):
    return jnp.where(mask, 1.0, 0.0).astype(bf16)


def total(values, axis):
    return jnp.sum(values, axis=axis, keepdims=True)


def members(step):
    return step, 15 - step, 7 - step, 8 + step


def fit_orders(step, s, d):
    js = members(step)
    u, v = (s[0] + s[1], s[2] + s[3]), (s[0] - s[1], s[2] - s[3])
    out = []
    for c in range(KEEP):
        if c % 2:
            terms = list(zip(js, d))
        elif c % 4:
            terms = [(js[0], v[0]), (js[2], v[1])]
        elif c % 8:
            terms = [(js[0], u[0] - u[1])]
        else:
            terms = [(js[0], u[0] + u[1])]
        value = None
        for j, term in terms:
            scaled = float(FIT[c, j]) * term
            value = scaled if value is None else value + scaled
        out.append(value)
    return out


def kernel(
    energies, triples_hbm, surfaces, pair_slot_hbm, singles_hbm, modals_hbm, mode_slot_hbm, weights_hbm, small_hbm,
    coefficients, energy_out, mean_out,
    triples, pair_slot, singles, modals, mode_slot, small,
    values, surf, weights, planes, acc, table, hits, answers, arrived, pair_t, padded, message, received,
    modes_in, exp_modals, deep, moved, moments,
    load_sem, send_msg, recv_msg, send_ans, recv_ans, send_mom, recv_mom,
    *, devices, groups,
):
    number = triples_hbm.shape[1]
    needs = 3 * number
    pair_rows = surfaces.shape[0]
    mode_rows = modals_hbm.shape[0]
    modes = pair_slot_hbm.shape[0]
    capacity = needs // devices
    cap = answers.shape[1]
    slots = devices * cap
    bands = -(-mode_rows // 8)
    offset = 2 * KEEP * bands
    width = moved.shape[2]
    everyone = devices * groups
    me = lax.axis_index("dev")
    group = lax.axis_index("grp")
    flat = group * devices + me

    pairs = [
        (triples_hbm, triples), (pair_slot_hbm, pair_slot), (singles_hbm, singles),
        (modals_hbm, modals), (mode_slot_hbm, mode_slot), (small_hbm, small),
        (weights_hbm, weights), (surfaces, surf),
    ]
    part = energies.shape[1] // CHUNKS
    for i in range(CHUNKS):
        span = pl.ds(i * part, part)
        pairs.append((energies.at[:, span], values.at[:, span]))
    loads = [pltpu.make_async_copy(source, target, load_sem.at[i]) for i, (source, target) in enumerate(pairs)]
    for load in loads[:SMALLS]:
        load.start()

    barrier = pltpu.get_barrier_semaphore()

    def each_peer(action):
        def step(k, carry):
            action(lax.rem(me + k, devices))
            return carry

        lax.fori_loop(1, devices, step, 0)

    def each_other(action):
        each_peer(lambda peer: action(group, peer))
        for k in range(1, groups):
            there = lax.rem(group + k, groups)
            action(there, me)
            each_peer(lambda peer: action(there, peer))

    each_other(
        lambda there, peer: pl.semaphore_signal(barrier, inc=1, device_id=(there, peer), device_id_type=MESH)
    )
    for load in loads[SMALLS:]:
        load.start()
    for load in loads[:SMALLS]:
        load.wait()

    padded[...] = jnp.zeros_like(padded)
    padded[1, 0:modes, 0:modes] = pair_slot[...].astype(f32)
    padded[2, 0:1, 0:modes] = mode_slot[...].astype(f32)
    picks = [triples[p : p + 1, :] for p in range(3)]
    rows = iota((LANES, number), 0)
    on = [rows == pick for pick in picks]
    on_hot = [ones_at(x) for x in on]
    pair_ints = padded[1].astype(jnp.int32)
    first_two = jnp.concatenate(on_hot[:2], axis=1)
    lines = 128.0 * nn((pair_ints >> 7).astype(f32).astype(bf16), first_two)
    lines = lines + nn((pair_ints & 127).astype(f32).astype(bf16), first_two)
    chosen = [
        total(jnp.where(on[1], lines[:, :number], 0.0), 0),
        total(jnp.where(on[2], lines[:, :number], 0.0), 0),
        total(jnp.where(on[2], lines[:, number:], 0.0), 0),
    ]
    flips = [picks[0] > picks[1], picks[0] > picks[2], picks[1] > picks[2]]
    pair_ids = (jnp.concatenate(chosen, axis=1) + 0.5).astype(jnp.int32)
    holders = iota((devices, needs), 0)
    held = (pair_ids >= holders * pair_rows) & (pair_ids < (holders + 1) * pair_rows)
    held_hot = ones_at(held)
    owner = total(jnp.where(held, holders, 0), 0)
    local = pair_ids - owner * pair_rows
    before = ones_at(iota((number, number), 0) < iota((number, number), 1))
    seen = jnp.zeros((devices, 1), f32)
    ranks = []
    for p in range(3):
        block = held_hot[:, p * number : (p + 1) * number]
        mine = held[:, p * number : (p + 1) * number]
        ranks.append(total(jnp.where(mine, nn(block, before) + seen, 0.0), 0))
        seen = seen + total(jnp.where(mine, 1.0, 0.0), 1)
    rank = (jnp.concatenate(ranks, axis=1) + 0.5).astype(jnp.int32)
    place = owner * cap + rank
    at_rank = ones_at(iota((LANES, needs), 0) == rank)
    coarse = jnp.where(held, (local >> 4).astype(f32), 0.0).astype(bf16)
    fine = jnp.where(held, (local & 15).astype(f32), 0.0).astype(bf16)
    requests = 16.0 * nt(coarse, at_rank) + nt(fine, at_rank)

    modes_in[...] = jnp.zeros_like(modes_in)
    modes_in[0:mode_rows, 0 : G * S] = modals[...]
    modes_in[0:mode_rows, G * S : G * S + G] = singles[...]
    every = modes_in[:, 0 : G * S]
    spread = small[:, 0 : G * S]
    lane = iota((KEEP, G * S), 1)
    ground_weights = jnp.where((lane & (S - 1)) == 0, spread, 0.0)
    ground_here = nt(every * every, ground_weights, highest)
    single_here = nt(modes_in[:, G * S : G * S + G], small[:, G * S : G * S + G], highest)
    padded[3, 0 : modes_in.shape[0], 0:KEEP] = ground_here
    padded[3, 0 : modes_in.shape[0], KEEP : 2 * KEEP] = single_here
    base = padded[3, 0:8, :]
    for q in range(1, bands):
        base = base + pltpu.roll(padded[3, 8 * q : 8 * q + 8, :], 2 * KEEP * q, 1)
    asked = pltpu.roll(requests, offset, 1)
    top = iota((8, LANES), 0) == 0
    for p in range(devices):
        message[p] = base + jnp.where(top, asked[p : p + 1, :], 0.0)
    received[me] = message[me]

    pl.semaphore_wait(barrier, everyone - 1)

    def message_copy(peer, slot):
        return pltpu.make_async_remote_copy(
            src_ref=message.at[peer], dst_ref=received.at[slot],
            send_sem=send_msg.at[peer], recv_sem=recv_msg.at[slot],
            device_id=(group, peer), device_id_type=MESH,
        )

    def answer_copy(peer, slot):
        return pltpu.make_async_remote_copy(
            src_ref=answers.at[peer], dst_ref=arrived.at[slot],
            send_sem=send_ans.at[peer], recv_sem=recv_ans.at[slot],
            device_id=(group, peer), device_id_type=MESH,
        )

    each_peer(lambda peer: message_copy(peer, me).start())

    loads[SMALLS].wait()
    loads[SMALLS + 1].wait()
    w_high = weights[0:AREA, :]
    w_low = weights[AREA : 2 * AREA, :]
    table_rows = table.shape[1]
    done = 0
    while done < table_rows:
        size = min(256, table_rows - done)
        have = min(size, pair_rows - done)
        whole = have // 16 * 16
        pieces = []
        if whole:
            pieces.append(surf[done : done + whole, :])
        if size > whole:
            rest = jnp.zeros((size - whole, G * G), f32)
            if have > whole:
                tail = jnp.concatenate(
                    [surf[done + whole : done + have, :], jnp.zeros((16 - (have - whole), G * G), f32)], axis=0
                )
                pieces.append(tail)
                rest = jnp.zeros((size - whole - 16, G * G), f32)
            if rest.shape[0]:
                pieces.append(None)
        at = done
        for piece in pieces:
            if piece is None:
                table[:, at : done + size, :] = jnp.zeros((2, done + size - at, AREA), bf16)
                continue
            high, low = split(piece)
            fitted = nt(high, w_high) + nt(high, w_low) + nt(low, w_high)
            count = piece.shape[0]
            part_high, part_low = split(fitted)
            table[0, at : at + count, :] = part_high
            table[1, at : at + count, :] = part_low
            at += count
        done += size

    for load in loads[SMALLS + 2 :]:
        load.wait()

    def inner_fit(step):
        for i, j in enumerate(members(step)):
            front = values[:, j * G * G : (j + 1) * G * G]
            back = values[:, (G - 1 - j) * G * G : (G - j) * G * G]
            both = jnp.concatenate([front, back], axis=0)
            plane = nt(weights[0:AREA, :], both) + nt(weights[AREA : 2 * AREA, :], both)
            planes[step % 2, i] = plane[:, :number] + plane[:, number:]
            planes[step % 2, 4 + i] = plane[:, :number] - plane[:, number:]

    def outer_fit(step):
        for block in range(AREA // 8):
            span = slice(block * 8, block * 8 + 8)
            sums = [planes[step % 2, i, span, :] for i in range(4)]
            differences = [planes[step % 2, 4 + i, span, :] for i in range(4)]
            for c, value in enumerate(fit_orders(step, sums, differences)):
                acc[c, span, :] = value if step == 0 else acc[c, span, :] + value

    for step in range(EARLY):
        inner_fit(step)
        if step:
            outer_fit(step - 1)

    each_peer(lambda peer: message_copy(me, peer).wait_recv())
    wanted = jnp.concatenate([received[p, 0:1, :] for p in range(devices)], axis=0)
    wanted = jnp.concatenate([wanted, jnp.zeros((LANES - devices, LANES), f32)], axis=0)
    wanted = (wanted.T[offset : offset + cap if offset + cap <= LANES else LANES, :] + 0.5).astype(jnp.int32)
    in_table = iota((capacity, table_rows), 1)
    if cap > capacity:
        hits[...] = jnp.zeros_like(hits)
    for p in range(devices):
        hits[p, 0:capacity, :] = ones_at(wanted[0:capacity, p : p + 1] == in_table)
    all_hits = hits[...].reshape(slots, table_rows)
    found = nn(all_hits, table[0]) + nn(all_hits, table[1])
    answers[...] = found.reshape(devices, cap, AREA)
    arrived[me] = answers[me]
    each_peer(lambda peer: answer_copy(peer, me).start())

    modes_hot = jnp.concatenate(on_hot, axis=1)
    slot_ids = (nn(padded[2, 0:8, :].astype(bf16), modes_hot)[0:1, :] + 0.5).astype(jnp.int32)
    homes = iota((devices, needs), 0)
    home = (slot_ids >= homes * mode_rows) & (slot_ids < (homes + 1) * mode_rows)
    home_row = total(jnp.where(home, homes, 0), 0)
    at_home = slot_ids - home_row * mode_rows
    spot = home_row * 8 + (at_home & 7)
    spot_hot = ones_at(iota((devices * 8, needs), 0) == spot)
    tables_high, tables_low = split(received[...].reshape(devices * 8, LANES))
    looked = tn(tables_high, spot_hot) + tn(tables_low, spot_hot)
    band = at_home >> 3
    taken = jnp.where(band == 0, looked[0 : 2 * KEEP], 0.0)
    for q in range(1, bands):
        taken = jnp.where(band == q, looked[2 * KEEP * q : 2 * KEEP * (q + 1)], taken)
    ground = [taken[0:KEEP, p * number : (p + 1) * number] for p in range(3)]
    single = [taken[KEEP : 2 * KEEP, p * number : (p + 1) * number] for p in range(3)]

    for step in range(EARLY, STEPS):
        inner_fit(step)
        outer_fit(step - 1)
    outer_fit(STEPS - 1)

    each_peer(lambda peer: answer_copy(me, peer).wait_recv())
    place_hot = ones_at(iota((slots, needs), 0) == place)
    arrived_high, arrived_low = split(arrived[...].reshape(slots, AREA))
    ordered = tn(arrived_high, place_hot) + tn(arrived_low, place_hot)
    for p in range(3):
        pair_t[p] = ordered[:, p * number : (p + 1) * number]

    def pair_rows_of(p, c):
        straight = pair_t[p, c * KEEP : (c + 1) * KEEP, :]
        turned_rows = pair_t[p, pl.ds(c, KEEP, stride=KEEP), :]
        return jnp.where(flips[p], turned_rows, straight)

    first_row = iota((KEEP, number), 0) == 0
    for c in range(KEEP):
        along_d = pair_rows_of(0, c)
        along_e = pair_rows_of(1, c) + jnp.where(first_row, single[0][c : c + 1, :], 0.0)
        if c == 0:
            along_d = along_d + single[1]
            along_e = along_e + single[2]
            for d in range(KEEP):
                acc[0, d * KEEP : (d + 1) * KEEP, :] -= pair_rows_of(2, d)
        acc[c, pl.ds(0, KEEP, stride=KEEP), :] -= along_d
        acc[c, 0:KEEP, :] -= along_e

    low3, high3 = ground[2][0:8], ground[2][8:16]
    rows1 = [ground[0][c : c + 1, :] for c in range(KEEP)]
    partial1 = [jnp.zeros((8, number), f32) for _ in range(KEEP)]
    field2 = []
    field3 = [jnp.zeros((8, number), f32) for _ in range(2)]
    for d in range(KEEP):
        row2 = ground[1][d : d + 1, :]
        inner = jnp.zeros((8, number), f32)
        for h, part3 in enumerate((low3, high3)):
            weight = row2 * part3
            mixed = jnp.zeros((8, number), f32)
            for c in range(KEEP):
                value = acc[c, d * KEEP + 8 * h : d * KEEP + 8 * h + 8, :]
                partial1[c] = partial1[c] + value * weight
                mixed = mixed + value * rows1[c]
            inner = inner + mixed * part3
            field3[h] = field3[h] + mixed * row2
        field2.append(total(inner, 0))
    field1 = jnp.concatenate([total(x, 0) for x in partial1], axis=0)
    field2 = jnp.concatenate(field2, axis=0)
    field3 = jnp.concatenate(field3, axis=0)
    energy_out[...] = total(field1 * ground[0], 0)

    fields = jnp.concatenate([field1, field2, field3], axis=1)
    fields = jnp.concatenate([fields] * (width // KEEP), axis=0)
    of_row = (iota((width, needs), 0) >> 4) == at_home
    fields_high, fields_low = split(jnp.where(of_row, fields, 0.0))
    home_hot = ones_at(home)
    sums = nt(home_hot, fields_high) + nt(home_hot, fields_low)
    for p in range(devices):
        moved[p] = sums[p : p + 1, :]
    moments[flat] = moved[me]

    def moment_copy(there, peer, slot):
        return pltpu.make_async_remote_copy(
            src_ref=moved.at[peer], dst_ref=moments.at[slot],
            send_sem=send_mom.at[there * devices + peer], recv_sem=recv_mom.at[slot],
            device_id=(there, peer), device_id_type=MESH,
        )

    each_other(lambda there, peer: moment_copy(there, peer, flat).start())

    for c in range(KEEP):
        coefficients[:, c * AREA : (c + 1) * AREA] = acc[c].T.astype(bf16)

    rows16 = modes_in.shape[0]
    for g in range(G):
        exp_modals[g * rows16 : (g + 1) * rows16, 0:S] = modes_in[:, g * S : (g + 1) * S]
    pieces = exp_modals[:, 0:S]
    columns = iota((S, AREA), 1)
    index = iota((S, AREA), 0)
    by_a = jnp.where((columns >> 4) == index, 1.0, 0.0)
    by_b = jnp.where((columns & (S - 1)) == index, 1.0, 0.0)
    piece_high, piece_low = split(pieces)
    by_a, by_b = by_a.astype(bf16), by_b.astype(bf16)
    products = (nn(piece_high, by_a) + nn(piece_low, by_a)) * (nn(piece_high, by_b) + nn(piece_low, by_b))
    products_high, products_low = split(products)
    tall = jnp.concatenate([spread] * (width // KEEP), axis=0)
    own_row = (iota(tall.shape, 1) & (rows16 - 1)) == (iota(tall.shape, 0) >> 4)
    tall_high, tall_low = split(jnp.where(own_row, tall, 0.0))
    deep[...] = nn(tall_high, products_high) + nn(tall_high, products_low) + nn(tall_low, products_high)

    each_other(lambda there, peer: moment_copy(group, me, there * devices + peer).wait_recv())
    summed = moments[0]
    for k in range(1, everyone):
        summed = summed + moments[k]
    chosen_rows = (iota((rows16, width), 1) >> 4) == iota((rows16, width), 0)
    mean = nn(jnp.where(chosen_rows, summed, 0.0), deep[...], highest)
    mean_out[...] = mean[0:mode_rows, :]

    each_peer(lambda peer: message_copy(peer, me).wait_send())
    each_peer(lambda peer: answer_copy(peer, me).wait_send())
    each_other(lambda there, peer: moment_copy(there, peer, flat).wait_send())


def write_kernel(coefficients, energy, mean, coefficients_out, energy_out, mean_out, sems):
    copies = [
        pltpu.make_async_copy(source, target, sems.at[i])
        for i, (source, target) in enumerate(
            [(coefficients, coefficients_out), (energy, energy_out), (mean, mean_out)]
        )
    ]
    for copy in copies:
        copy.start()
    for copy in copies:
        copy.wait()


def body(energies, triples, pair_surfaces, pair_slot, single_surfaces, modals, mode_slot):
    devices = lax.axis_size("dev")
    groups = lax.axis_size("grp")
    number = triples.shape[0]
    pair_rows = pair_surfaces.shape[0]
    mode_rows = modals.shape[0]
    cap = round_up(3 * number // devices, 16)
    table_rows = round_up(pair_rows, 256)
    width = round_up(mode_rows * KEEP, LANES)
    rows16 = 16
    everyone = devices * groups
    vmem = pl.BlockSpec(memory_space=pltpu.VMEM)
    hbm = pl.BlockSpec(memory_space=pltpu.HBM)
    small_shapes = [
        (triples.shape[::-1], jnp.int32), (pair_slot.shape, jnp.int32), (single_surfaces.shape, f32),
        (modals.shape, f32), ((1, mode_slot.shape[0]), jnp.int32), (SMALL.shape, f32),
    ]
    results = [
        jax.ShapeDtypeStruct((number, KEEP * AREA), bf16),
        jax.ShapeDtypeStruct((1, number), f32),
        jax.ShapeDtypeStruct((mode_rows, S * S), f32),
    ]
    in_vmem = pl.pallas_call(
        functools.partial(kernel, devices=devices, groups=groups),
        in_specs=[hbm] * 9,
        out_specs=[vmem, vmem, vmem],
        out_shape=results,
        scratch_shapes=[
            *[pltpu.VMEM(shape, kind) for shape, kind in small_shapes],
            pltpu.VMEM(energies.shape, bf16),
            pltpu.VMEM(pair_surfaces.shape, f32),
            pltpu.VMEM(WEIGHTS.shape, bf16),
            pltpu.VMEM((2, 8, AREA, number), f32),
            pltpu.VMEM((KEEP, AREA, number), f32),
            pltpu.VMEM((2, table_rows, AREA), bf16),
            pltpu.VMEM((devices, cap, table_rows), bf16),
            pltpu.VMEM((devices, cap, AREA), f32),
            pltpu.VMEM((devices, cap, AREA), f32),
            pltpu.VMEM((3, AREA, number), f32),
            pltpu.VMEM((4, LANES, LANES), f32),
            pltpu.VMEM((devices, 8, LANES), f32),
            pltpu.VMEM((devices, 8, LANES), f32),
            pltpu.VMEM((rows16, SMALL.shape[1]), f32),
            pltpu.VMEM((G * rows16, LANES), f32),
            pltpu.VMEM((width, AREA), f32),
            pltpu.VMEM((devices, 1, width), f32),
            pltpu.VMEM((everyone, 1, width), f32),
            pltpu.SemaphoreType.DMA((SMALLS + 2 + CHUNKS,)),
            pltpu.SemaphoreType.DMA((devices,)),
            pltpu.SemaphoreType.DMA((devices,)),
            pltpu.SemaphoreType.DMA((devices,)),
            pltpu.SemaphoreType.DMA((devices,)),
            pltpu.SemaphoreType.DMA((everyone,)),
            pltpu.SemaphoreType.DMA((everyone,)),
        ],
        compiler_params=pltpu.CompilerParams(
            collective_id=0, has_side_effects=True, vmem_limit_bytes=32 * 1024 * 1024
        ),
    )(
        *[
            pltpu.with_memory_space_constraint(x, pltpu.HBM)
            for x in (
                energies, triples.T, pair_surfaces, pair_slot, single_surfaces, modals, mode_slot.reshape(1, -1),
                jnp.asarray(WEIGHTS), jnp.asarray(SMALL),
            )
        ]
    )
    coefficients, energy, mean = pl.pallas_call(
        write_kernel,
        in_specs=[vmem] * 3,
        out_specs=[hbm] * 3,
        out_shape=results,
        scratch_shapes=[pltpu.SemaphoreType.DMA((3,))],
        compiler_params=pltpu.CompilerParams(vmem_limit_bytes=1024 * 1024),
    )(*in_vmem)
    return coefficients, energy.reshape(number), mean


def solution(mesh):
    in_specs = (
        P(("grp", "dev"), None),
        P(("grp", "dev"), None),
        P("dev", None),
        P(),
        P("dev", None),
        P("dev", None),
        P(),
    )
    out_specs = (P(("grp", "dev"), None), P(("grp", "dev")), P("dev", None))
    return jax.shard_map(body, mesh=mesh, in_specs=in_specs, out_specs=out_specs, check_vma=False)
```

```python
import functools

import jax
import jax.numpy as jnp
import numpy as np
from jax import lax
from jax.experimental import pallas as pl
from jax.experimental.pallas import tpu as pltpu
from jax.sharding import PartitionSpec as P

G = 32
KEEP = 16
S = 16
AREA = KEEP * KEEP
HALF = G // 2
LANES = 128
STEPS = 4
CHUNKS = 8
SMALLS = 6
MESH = pl.DeviceIdType.MESH
f32 = jnp.float32
bf16 = jnp.bfloat16
highest = lax.Precision.HIGHEST


def np_tables():
    orders = np.arange(KEEP, dtype=np.float64)
    points = np.arange(G, dtype=np.float64) + 0.5
    cosines = np.cos(np.pi * orders[:, None] * points[None, :] / G)
    weights = np.where(orders == 0, 1.0, 2.0) / G
    return cosines, weights[:, None] * cosines


COS, FIT = np_tables()


def split_np(values):
    values = np.asarray(values, np.float32)
    high = values.astype(jnp.bfloat16)
    return high, (values - high.astype(np.float32)).astype(jnp.bfloat16)


INNER = np.einsum("dh,el->dehl", FIT, FIT).reshape(AREA, G * G)
WEIGHTS = np.concatenate(split_np(INNER), axis=0)
SMALL = np.concatenate([np.repeat(COS, S, axis=1), FIT, np.zeros((KEEP, LANES - G))], axis=1).astype(np.float32)


def round_up(value, step):
    return -(-value // step) * step


def iota(shape, axis):
    return lax.broadcasted_iota(jnp.int32, shape, axis)


def nn(a, b, precision=None):
    return lax.dot_general(a, b, (((1,), (0,)), ((), ())), precision=precision, preferred_element_type=f32)


def nt(a, b, precision=None):
    return lax.dot_general(a, b, (((1,), (1,)), ((), ())), precision=precision, preferred_element_type=f32)


def tn(a, b, precision=None):
    return lax.dot_general(a, b, (((0,), (0,)), ((), ())), precision=precision, preferred_element_type=f32)


def split(values):
    high = values.astype(bf16)
    return high, (values - high.astype(f32)).astype(bf16)


def ones_at(mask):
    return jnp.where(mask, 1.0, 0.0).astype(bf16)


def total(values, axis):
    return jnp.sum(values, axis=axis, keepdims=True)


def members(step):
    return step, 15 - step, 7 - step, 8 + step


def fit_orders(step, s, d):
    js = members(step)
    u, v = (s[0] + s[1], s[2] + s[3]), (s[0] - s[1], s[2] - s[3])
    out = []
    for c in range(KEEP):
        if c % 2:
            terms = list(zip(js, d))
        elif c % 4:
            terms = [(js[0], v[0]), (js[2], v[1])]
        elif c % 8:
            terms = [(js[0], u[0] - u[1])]
        else:
            terms = [(js[0], u[0] + u[1])]
        value = None
        for j, term in terms:
            scaled = float(FIT[c, j]) * term
            value = scaled if value is None else value + scaled
        out.append(value)
    return out


def kernel(
    energies, triples_hbm, surfaces, pair_slot_hbm, singles_hbm, modals_hbm, mode_slot_hbm, weights_hbm, small_hbm,
    coefficients, energy_out, mean_out,
    triples, pair_slot, singles, modals, mode_slot, small,
    values, surf, weights, planes, acc, table, hits, answers, arrived, pair_t, padded, message, received,
    modes_of, mode_table, modes_in, exp_modals, deep, moved, moments,
    load_sem, send_msg, recv_msg, send_ans, recv_ans, send_mom, recv_mom,
    *, devices, groups,
):
    number = triples_hbm.shape[1]
    needs = 3 * number
    pair_rows = surfaces.shape[0]
    mode_rows = modals_hbm.shape[0]
    modes = pair_slot_hbm.shape[0]
    capacity = needs // devices
    cap = answers.shape[1]
    slots = devices * cap
    bands = -(-mode_rows // 8)
    held_rows = 8 * bands
    spots_all = devices * held_rows
    offset = 2 * KEEP * bands
    width = moved.shape[2]
    everyone = devices * groups
    me = lax.axis_index("dev")
    group = lax.axis_index("grp")
    flat = group * devices + me

    pairs = [
        (triples_hbm, triples), (pair_slot_hbm, pair_slot), (singles_hbm, singles),
        (modals_hbm, modals), (mode_slot_hbm, mode_slot), (small_hbm, small),
        (weights_hbm, weights), (surfaces, surf),
    ]
    part = energies.shape[1] // CHUNKS
    for i in range(CHUNKS):
        span = pl.ds(i * part, part)
        pairs.append((energies.at[:, span], values.at[:, span]))
    loads = [pltpu.make_async_copy(source, target, load_sem.at[i]) for i, (source, target) in enumerate(pairs)]
    for load in loads[:SMALLS]:
        load.start()

    barrier = pltpu.get_barrier_semaphore()

    def each_peer(action):
        def step(k, carry):
            action(lax.rem(me + k, devices))
            return carry

        lax.fori_loop(1, devices, step, 0)

    def each_other(action):
        each_peer(lambda peer: action(group, peer))
        for k in range(1, groups):
            there = lax.rem(group + k, groups)
            action(there, me)
            each_peer(lambda peer: action(there, peer))

    each_other(
        lambda there, peer: pl.semaphore_signal(barrier, inc=1, device_id=(there, peer), device_id_type=MESH)
    )
    for load in loads[SMALLS:]:
        load.start()
    for load in loads[:SMALLS]:
        load.wait()

    padded[...] = jnp.zeros_like(padded)
    padded[1, 0:modes, 0:modes] = pair_slot[...].astype(f32)
    padded[2, 0:1, 0:modes] = mode_slot[...].astype(f32)
    picks = [triples[p : p + 1, :] for p in range(3)]
    rows = iota((LANES, number), 0)
    on = [rows == pick for pick in picks]
    on_hot = [ones_at(x) for x in on]
    pair_ints = padded[1].astype(jnp.int32)
    first_two = jnp.concatenate(on_hot[:2], axis=1)
    lines = 128.0 * nn((pair_ints >> 7).astype(f32).astype(bf16), first_two)
    lines = lines + nn((pair_ints & 127).astype(f32).astype(bf16), first_two)
    chosen = [
        total(jnp.where(on[1], lines[:, :number], 0.0), 0),
        total(jnp.where(on[2], lines[:, :number], 0.0), 0),
        total(jnp.where(on[2], lines[:, number:], 0.0), 0),
    ]
    flips = [picks[0] > picks[1], picks[0] > picks[2], picks[1] > picks[2]]
    pair_ids = (jnp.concatenate(chosen, axis=1) + 0.5).astype(jnp.int32)
    holders = iota((devices, needs), 0)
    held = (pair_ids >= holders * pair_rows) & (pair_ids < (holders + 1) * pair_rows)
    held_hot = ones_at(held)
    owner = total(jnp.where(held, holders, 0), 0)
    local = pair_ids - owner * pair_rows
    before = ones_at(iota((number, number), 0) < iota((number, number), 1))
    seen = jnp.zeros((devices, 1), f32)
    ranks = []
    for p in range(3):
        block = held_hot[:, p * number : (p + 1) * number]
        mine = held[:, p * number : (p + 1) * number]
        ranks.append(total(jnp.where(mine, nn(block, before) + seen, 0.0), 0))
        seen = seen + total(jnp.where(mine, 1.0, 0.0), 1)
    rank = (jnp.concatenate(ranks, axis=1) + 0.5).astype(jnp.int32)
    place = owner * cap + rank
    at_rank = ones_at(iota((LANES, needs), 0) == rank)
    modes_hot = jnp.concatenate(on_hot, axis=1)
    slot_ids = (nn(padded[2, 0:8, :].astype(bf16), modes_hot)[0:1, :] + 0.5).astype(jnp.int32)
    homes = iota((devices, needs), 0)
    home_row = total(jnp.where(slot_ids >= (homes + 1) * mode_rows, 1, 0), 0)
    spot = home_row * held_rows + slot_ids - home_row * mode_rows
    spots = [spot[:, p * number : (p + 1) * number] for p in range(3)]
    lower, upper, third = [], [], []
    for p, (one, two, three) in enumerate(((0, 1, 2), (0, 2, 1), (1, 2, 0))):
        lower.append(jnp.where(flips[p], spots[two], spots[one]))
        upper.append(jnp.where(flips[p], spots[one], spots[two]))
        third.append(spots[three])
    told = [local >> 4, local & 15] + [jnp.concatenate(x, axis=1) for x in (lower, upper, third)]
    told = [jnp.where(held, x.astype(f32), 0.0).astype(bf16) for x in told]
    sorted_told = nt(jnp.concatenate(told, axis=0), at_rank)
    parts = [sorted_told[f * devices : (f + 1) * devices, :] for f in range(5)]
    requests = [16.0 * parts[0] + parts[1]] + parts[2:]

    modes_in[...] = jnp.zeros_like(modes_in)
    modes_in[0:mode_rows, 0 : G * S] = modals[...]
    modes_in[0:mode_rows, G * S : G * S + G] = singles[...]
    every = modes_in[:, 0 : G * S]
    spread = small[:, 0 : G * S]
    lane = iota((KEEP, G * S), 1)
    ground_weights = jnp.where((lane & (S - 1)) == 0, spread, 0.0)
    ground_here = nt(every * every, ground_weights, highest)
    single_here = nt(modes_in[:, G * S : G * S + G], small[:, G * S : G * S + G], highest)
    padded[3, 0 : modes_in.shape[0], 0:KEEP] = ground_here
    padded[3, 0 : modes_in.shape[0], KEEP : 2 * KEEP] = single_here
    base = padded[3, 0:8, :]
    for q in range(1, bands):
        base = base + pltpu.roll(padded[3, 8 * q : 8 * q + 8, :], 2 * KEEP * q, 1)
    asked = [pltpu.roll(x, offset, 1) for x in requests]
    blank = jnp.zeros((8 - len(asked), LANES), f32)
    for p in range(devices):
        message[p] = base + jnp.concatenate([x[p : p + 1, :] for x in asked] + [blank], axis=0)
    received[me] = message[me]

    pl.semaphore_wait(barrier, everyone - 1)

    def message_copy(peer, slot):
        return pltpu.make_async_remote_copy(
            src_ref=message.at[peer], dst_ref=received.at[slot],
            send_sem=send_msg.at[peer], recv_sem=recv_msg.at[slot],
            device_id=(group, peer), device_id_type=MESH,
        )

    def answer_copy(peer, slot):
        return pltpu.make_async_remote_copy(
            src_ref=answers.at[peer], dst_ref=arrived.at[slot],
            send_sem=send_ans.at[peer], recv_sem=recv_ans.at[slot],
            device_id=(group, peer), device_id_type=MESH,
        )

    each_peer(lambda peer: message_copy(peer, me).start())

    loads[SMALLS].wait()
    loads[SMALLS + 1].wait()
    w_high = weights[0:AREA, :]
    w_low = weights[AREA : 2 * AREA, :]
    table_rows = table.shape[1]
    done = 0
    while done < table_rows:
        size = min(256, table_rows - done)
        have = min(size, pair_rows - done)
        whole = have // 16 * 16
        pieces = []
        if whole:
            pieces.append(surf[done : done + whole, :])
        if size > whole:
            rest = jnp.zeros((size - whole, G * G), f32)
            if have > whole:
                tail = jnp.concatenate(
                    [surf[done + whole : done + have, :], jnp.zeros((16 - (have - whole), G * G), f32)], axis=0
                )
                pieces.append(tail)
                rest = jnp.zeros((size - whole - 16, G * G), f32)
            if rest.shape[0]:
                pieces.append(None)
        at = done
        for piece in pieces:
            if piece is None:
                table[:, at : done + size, :] = jnp.zeros((2, done + size - at, AREA), bf16)
                continue
            high, low = split(piece)
            fitted = nt(high, w_high) + nt(high, w_low) + nt(low, w_high)
            count = piece.shape[0]
            part_high, part_low = split(fitted)
            table[0, at : at + count, :] = part_high
            table[1, at : at + count, :] = part_low
            at += count
        done += size

    each_peer(lambda peer: message_copy(me, peer).wait_recv())
    wanted = [received[p, f : f + 1, :] for f in range(4) for p in range(devices)]
    if 4 * devices < LANES:
        wanted.append(jnp.zeros((LANES - 4 * devices, LANES), f32))
    wanted = (jnp.concatenate(wanted, axis=0).T[offset : offset + cap, :] + 0.5).astype(jnp.int32)
    in_table = iota((capacity, table_rows), 1)
    if cap > capacity:
        hits[...] = jnp.zeros_like(hits)
        modes_of[...] = jnp.zeros_like(modes_of)
    for p in range(devices):
        hits[p, 0:capacity, :] = ones_at(wanted[0:capacity, p : p + 1] == in_table)
    all_hits = hits[...].reshape(slots, table_rows)
    found = nn(all_hits, table[0]) + nn(all_hits, table[1])
    answers[...] = found.reshape(devices, cap, AREA)
    arrived[me] = answers[me]
    each_peer(lambda peer: answer_copy(peer, me).start())

    sent = received[...].reshape(devices * 8, LANES)
    for q in range(bands):
        turned = pltpu.roll(sent, LANES - 2 * KEEP * q, 1) if q else sent
        mode_table[:, 8 * q : 8 * q + 8, :] = turned.reshape(devices, 8, LANES)
    mode_rows_all = mode_table[...].reshape(spots_all, LANES)[:, 0 : 2 * KEEP]
    tables_high, tables_low = split(mode_rows_all)
    spot_hot = ones_at(iota((spots_all, needs), 0) == spot)
    taken = tn(tables_high, spot_hot) + tn(tables_low, spot_hot)
    ground = [taken[0:KEEP, p * number : (p + 1) * number] for p in range(3)]
    single = [taken[KEEP : 2 * KEEP, p * number : (p + 1) * number] for p in range(3)]

    in_spots = iota((capacity, spots_all), 1)
    for f in range(3):
        for p in range(devices):
            column = wanted[0:capacity, (f + 1) * devices + p : (f + 1) * devices + p + 1]
            modes_of[f, p, 0:capacity, :] = ones_at(column == in_spots)
    columns = iota((KEEP, AREA), 1)
    index = iota((KEEP, AREA), 0)
    by_first = ones_at((columns >> 4) == index)
    by_second = ones_at((columns & (KEEP - 1)) == index)
    by_zero = ones_at(index == 0)
    hot = [modes_of[f].reshape(slots, spots_all) for f in range(3)]

    def spread_modes(which, pattern):
        wide_high, wide_low = split(nn(tables_high[:, 0:KEEP], pattern) + nn(tables_low[:, 0:KEEP], pattern))
        return nn(hot[which], wide_high) + nn(hot[which], wide_low)

    def fold_orders(values, pattern):
        high, low = split(values)
        return nt(high, pattern) + nt(low, pattern)

    ground_lower = spread_modes(0, by_first)
    ground_upper = spread_modes(1, by_second)
    scaled = found * spread_modes(2, by_zero)
    takes = [
        fold_orders(scaled * ground_upper, by_first),
        fold_orders(scaled * ground_lower, by_second),
        fold_orders(found * ground_upper * ground_lower, by_zero),
    ]
    owed = jnp.zeros((spots_all, KEEP), f32)
    for f in range(3):
        high, low = split(takes[f])
        owed = owed + tn(hot[f], high) + tn(hot[f], low)

    for load in loads[SMALLS + 2 :]:
        load.wait()

    def inner_fit(step):
        for i, j in enumerate(members(step)):
            front = values[:, j * G * G : (j + 1) * G * G]
            back = values[:, (G - 1 - j) * G * G : (G - j) * G * G]
            both = jnp.concatenate([front, back], axis=0)
            plane = nt(weights[0:AREA, :], both) + nt(weights[AREA : 2 * AREA, :], both)
            planes[step % 2, i] = plane[:, :number] + plane[:, number:]
            planes[step % 2, 4 + i] = plane[:, :number] - plane[:, number:]

    def outer_fit(step):
        for block in range(AREA // 8):
            span = slice(block * 8, block * 8 + 8)
            sums = [planes[step % 2, i, span, :] for i in range(4)]
            differences = [planes[step % 2, 4 + i, span, :] for i in range(4)]
            for c, value in enumerate(fit_orders(step, sums, differences)):
                acc[c, span, :] = value if step == 0 else acc[c, span, :] + value

    for step in range(STEPS):
        inner_fit(step)
        if step:
            outer_fit(step - 1)
    outer_fit(STEPS - 1)

    first_row = iota((KEEP, number), 0) == 0
    for c in range(KEEP):
        here = jnp.where(first_row, single[0][c : c + 1, :], 0.0)
        acc[c, 0:KEEP, :] -= here + single[2] if c == 0 else here
    acc[0, pl.ds(0, KEEP, stride=KEEP), :] -= single[1]
    low3, high3 = ground[2][0:8], ground[2][8:16]
    rows1 = [ground[0][c : c + 1, :] for c in range(KEEP)]
    partial1 = [jnp.zeros((8, number), f32) for _ in range(KEEP)]
    field2 = []
    field3 = [jnp.zeros((8, number), f32) for _ in range(2)]
    for d in range(KEEP):
        row2 = ground[1][d : d + 1, :]
        inner = jnp.zeros((8, number), f32)
        for h, part3 in enumerate((low3, high3)):
            weight = row2 * part3
            mixed = jnp.zeros((8, number), f32)
            for c in range(KEEP):
                value = acc[c, d * KEEP + 8 * h : d * KEEP + 8 * h + 8, :]
                partial1[c] = partial1[c] + value * weight
                mixed = mixed + value * rows1[c]
            inner = inner + mixed * part3
            field3[h] = field3[h] + mixed * row2
        field2.append(total(inner, 0))
    field1 = jnp.concatenate([total(x, 0) for x in partial1], axis=0)
    field2 = jnp.concatenate(field2, axis=0)
    field3 = jnp.concatenate(field3, axis=0)
    energy = total(field1 * ground[0], 0)

    fields = jnp.concatenate([field1, field2, field3], axis=1)
    fields_high, fields_low = split(fields)
    by_spot = nt(spot_hot, fields_high) + nt(spot_hot, fields_low) - owed
    by_spot_high, by_spot_low = split(by_spot)
    repeat = ones_at((iota((KEEP, width), 1) & (KEEP - 1)) == iota((KEEP, width), 0))
    wide = nn(by_spot_high, repeat) + nn(by_spot_low, repeat)
    wide_row = iota((spots_all, width), 0) & (held_rows - 1)
    wide_high, wide_low = split(jnp.where(wide_row == (iota((spots_all, width), 1) >> 4), wide, 0.0))
    of_home = ones_at((iota((devices, spots_all), 1) // held_rows) == iota((devices, spots_all), 0))
    sums = nn(of_home, wide_high) + nn(of_home, wide_low)
    for p in range(devices):
        moved[p] = sums[p : p + 1, :]
    moments[flat] = moved[me]

    def moment_copy(there, peer, slot):
        return pltpu.make_async_remote_copy(
            src_ref=moved.at[peer], dst_ref=moments.at[slot],
            send_sem=send_mom.at[there * devices + peer], recv_sem=recv_mom.at[slot],
            device_id=(there, peer), device_id_type=MESH,
        )

    each_other(lambda there, peer: moment_copy(there, peer, flat).start())

    rows16 = modes_in.shape[0]
    for g in range(G):
        exp_modals[g * rows16 : (g + 1) * rows16, 0:S] = modes_in[:, g * S : (g + 1) * S]
    pieces = exp_modals[:, 0:S]
    piece_high, piece_low = split(pieces)
    products = (nn(piece_high, by_first) + nn(piece_low, by_first)) * (nn(piece_high, by_second) + nn(piece_low, by_second))
    products_high, products_low = split(products)
    tall = jnp.concatenate([spread] * (width // KEEP), axis=0)
    own_row = (iota(tall.shape, 1) & (rows16 - 1)) == (iota(tall.shape, 0) >> 4)
    tall_high, tall_low = split(jnp.where(own_row, tall, 0.0))
    deep[...] = nn(tall_high, products_high) + nn(tall_high, products_low) + nn(tall_low, products_high)

    each_peer(lambda peer: answer_copy(me, peer).wait_recv())
    place_hot = ones_at(iota((slots, needs), 0) == place)
    arrived_high, arrived_low = split(arrived[...].reshape(slots, AREA))
    ordered = tn(arrived_high, place_hot) + tn(arrived_low, place_hot)
    for p in range(3):
        pair_t[p] = ordered[:, p * number : (p + 1) * number]

    def pair_rows_of(p, c):
        straight = pair_t[p, c * KEEP : (c + 1) * KEEP, :]
        turned_rows = pair_t[p, pl.ds(c, KEEP, stride=KEEP), :]
        return jnp.where(flips[p], turned_rows, straight)

    for c in range(KEEP):
        acc[c, pl.ds(0, KEEP, stride=KEEP), :] -= pair_rows_of(0, c)
        acc[c, 0:KEEP, :] -= pair_rows_of(1, c)
        acc[0, c * KEEP : (c + 1) * KEEP, :] -= pair_rows_of(2, c)

    for p, (one, two, three) in enumerate(((0, 1, 2), (0, 2, 1), (1, 2, 0))):
        ground_low = jnp.where(flips[p], ground[two], ground[one])
        ground_high = jnp.where(flips[p], ground[one], ground[two])
        share = jnp.zeros((KEEP, number), f32)
        for c in range(KEEP):
            share = share + pair_t[p, c * KEEP : (c + 1) * KEEP, :] * ground_low[c : c + 1, :]
        energy = energy - ground[three][0:1, :] * total(share * ground_high, 0)
    energy_out[...] = energy

    for c in range(KEEP):
        coefficients[:, c * AREA : (c + 1) * AREA] = acc[c].T.astype(bf16)

    each_other(lambda there, peer: moment_copy(group, me, there * devices + peer).wait_recv())
    summed = moments[0]
    for k in range(1, everyone):
        summed = summed + moments[k]
    chosen_rows = (iota((rows16, width), 1) >> 4) == iota((rows16, width), 0)
    mean = nn(jnp.where(chosen_rows, summed, 0.0), deep[...], highest)
    mean_out[...] = mean[0:mode_rows, :]

    each_peer(lambda peer: message_copy(peer, me).wait_send())
    each_peer(lambda peer: answer_copy(peer, me).wait_send())
    each_other(lambda there, peer: moment_copy(there, peer, flat).wait_send())


def write_kernel(coefficients, energy, mean, coefficients_out, energy_out, mean_out, sems):
    copies = [
        pltpu.make_async_copy(source, target, sems.at[i])
        for i, (source, target) in enumerate(
            [(coefficients, coefficients_out), (energy, energy_out), (mean, mean_out)]
        )
    ]
    for copy in copies:
        copy.start()
    for copy in copies:
        copy.wait()


def body(energies, triples, pair_surfaces, pair_slot, single_surfaces, modals, mode_slot):
    devices = lax.axis_size("dev")
    groups = lax.axis_size("grp")
    number = triples.shape[0]
    pair_rows = pair_surfaces.shape[0]
    mode_rows = modals.shape[0]
    cap = round_up(3 * number // devices, 16)
    table_rows = round_up(pair_rows, 256)
    width = round_up(mode_rows * KEEP, LANES)
    rows16 = 16
    held_rows = round_up(mode_rows, 8)
    spots_all = devices * held_rows
    everyone = devices * groups
    vmem = pl.BlockSpec(memory_space=pltpu.VMEM)
    hbm = pl.BlockSpec(memory_space=pltpu.HBM)
    small_shapes = [
        (triples.shape[::-1], jnp.int32), (pair_slot.shape, jnp.int32), (single_surfaces.shape, f32),
        (modals.shape, f32), ((1, mode_slot.shape[0]), jnp.int32), (SMALL.shape, f32),
    ]
    results = [
        jax.ShapeDtypeStruct((number, KEEP * AREA), bf16),
        jax.ShapeDtypeStruct((1, number), f32),
        jax.ShapeDtypeStruct((mode_rows, S * S), f32),
    ]
    in_vmem = pl.pallas_call(
        functools.partial(kernel, devices=devices, groups=groups),
        in_specs=[hbm] * 9,
        out_specs=[vmem, vmem, vmem],
        out_shape=results,
        scratch_shapes=[
            *[pltpu.VMEM(shape, kind) for shape, kind in small_shapes],
            pltpu.VMEM(energies.shape, bf16),
            pltpu.VMEM(pair_surfaces.shape, f32),
            pltpu.VMEM(WEIGHTS.shape, bf16),
            pltpu.VMEM((2, 8, AREA, number), f32),
            pltpu.VMEM((KEEP, AREA, number), f32),
            pltpu.VMEM((2, table_rows, AREA), bf16),
            pltpu.VMEM((devices, cap, table_rows), bf16),
            pltpu.VMEM((devices, cap, AREA), f32),
            pltpu.VMEM((devices, cap, AREA), f32),
            pltpu.VMEM((3, AREA, number), f32),
            pltpu.VMEM((4, LANES, LANES), f32),
            pltpu.VMEM((devices, 8, LANES), f32),
            pltpu.VMEM((devices, 8, LANES), f32),
            pltpu.VMEM((3, devices, cap, spots_all), bf16),
            pltpu.VMEM((devices, held_rows, LANES), f32),
            pltpu.VMEM((rows16, SMALL.shape[1]), f32),
            pltpu.VMEM((G * rows16, LANES), f32),
            pltpu.VMEM((width, AREA), f32),
            pltpu.VMEM((devices, 1, width), f32),
            pltpu.VMEM((everyone, 1, width), f32),
            pltpu.SemaphoreType.DMA((SMALLS + 2 + CHUNKS,)),
            pltpu.SemaphoreType.DMA((devices,)),
            pltpu.SemaphoreType.DMA((devices,)),
            pltpu.SemaphoreType.DMA((devices,)),
            pltpu.SemaphoreType.DMA((devices,)),
            pltpu.SemaphoreType.DMA((everyone,)),
            pltpu.SemaphoreType.DMA((everyone,)),
        ],
        compiler_params=pltpu.CompilerParams(
            collective_id=0, has_side_effects=True, vmem_limit_bytes=32 * 1024 * 1024
        ),
    )(
        *[
            pltpu.with_memory_space_constraint(x, pltpu.HBM)
            for x in (
                energies, triples.T, pair_surfaces, pair_slot, single_surfaces, modals, mode_slot.reshape(1, -1),
                jnp.asarray(WEIGHTS), jnp.asarray(SMALL),
            )
        ]
    )
    coefficients, energy, mean = pl.pallas_call(
        write_kernel,
        in_specs=[vmem] * 3,
        out_specs=[hbm] * 3,
        out_shape=results,
        scratch_shapes=[pltpu.SemaphoreType.DMA((3,))],
        compiler_params=pltpu.CompilerParams(vmem_limit_bytes=1024 * 1024),
    )(*in_vmem)
    return coefficients, energy.reshape(number), mean


def solution(mesh):
    in_specs = (
        P(("grp", "dev"), None),
        P(("grp", "dev"), None),
        P("dev", None),
        P(),
        P("dev", None),
        P("dev", None),
        P(),
    )
    out_specs = (P(("grp", "dev"), None), P(("grp", "dev")), P("dev", None))
    return jax.shard_map(body, mesh=mesh, in_specs=in_specs, out_specs=out_specs, check_vma=False)
```

```python
import functools

import jax
import jax.numpy as jnp
import numpy as np
from jax import lax
from jax.experimental import pallas as pl
from jax.experimental.pallas import tpu as pltpu
from jax.sharding import PartitionSpec as P

G = 32
KEEP = 16
S = 16
AREA = KEEP * KEEP
HALF = G // 2
LANES = 128
STEPS = 4
EARLY = 1
CHUNKS = 8
SMALLS = 6
MESH = pl.DeviceIdType.MESH
f32 = jnp.float32
bf16 = jnp.bfloat16
highest = lax.Precision.HIGHEST


def np_tables():
    orders = np.arange(KEEP, dtype=np.float64)
    points = np.arange(G, dtype=np.float64) + 0.5
    cosines = np.cos(np.pi * orders[:, None] * points[None, :] / G)
    weights = np.where(orders == 0, 1.0, 2.0) / G
    return cosines, weights[:, None] * cosines


COS, FIT = np_tables()


def split_np(values):
    values = np.asarray(values, np.float32)
    high = values.astype(jnp.bfloat16)
    return high, (values - high.astype(np.float32)).astype(jnp.bfloat16)


INNER = np.einsum("dh,el->dehl", FIT, FIT).reshape(AREA, G * G)
WEIGHTS = np.concatenate(split_np(INNER), axis=0)
SMALL = np.concatenate([np.repeat(COS, S, axis=1), FIT, np.zeros((KEEP, LANES - G))], axis=1).astype(np.float32)


def round_up(value, step):
    return -(-value // step) * step


def iota(shape, axis):
    return lax.broadcasted_iota(jnp.int32, shape, axis)


def nn(a, b, precision=None):
    return lax.dot_general(a, b, (((1,), (0,)), ((), ())), precision=precision, preferred_element_type=f32)


def nt(a, b, precision=None):
    return lax.dot_general(a, b, (((1,), (1,)), ((), ())), precision=precision, preferred_element_type=f32)


def tn(a, b, precision=None):
    return lax.dot_general(a, b, (((0,), (0,)), ((), ())), precision=precision, preferred_element_type=f32)


def split(values):
    high = values.astype(bf16)
    return high, (values - high.astype(f32)).astype(bf16)


def ones_at(mask):
    return jnp.where(mask, 1.0, 0.0).astype(bf16)


def total(values, axis):
    return jnp.sum(values, axis=axis, keepdims=True)


def members(step):
    return step, 15 - step, 7 - step, 8 + step


def fit_orders(step, s, d):
    js = members(step)
    u, v = (s[0] + s[1], s[2] + s[3]), (s[0] - s[1], s[2] - s[3])
    out = []
    for c in range(KEEP):
        if c % 2:
            terms = list(zip(js, d))
        elif c % 4:
            terms = [(js[0], v[0]), (js[2], v[1])]
        elif c % 8:
            terms = [(js[0], u[0] - u[1])]
        else:
            terms = [(js[0], u[0] + u[1])]
        value = None
        for j, term in terms:
            scaled = float(FIT[c, j]) * term
            value = scaled if value is None else value + scaled
        out.append(value)
    return out


def kernel(
    energies, triples_hbm, surfaces, pair_slot_hbm, singles_hbm, modals_hbm, mode_slot_hbm, weights_hbm, small_hbm,
    coefficients, energy_out, mean_out,
    triples, pair_slot, singles, modals, mode_slot, small,
    values, surf, weights, planes, acc, table, hits, answers, arrived, pair_t, padded, message, received,
    modes_of, mode_table, modes_in, exp_modals, deep, moved, moments,
    load_sem, send_msg, recv_msg, send_ans, recv_ans, send_mom, recv_mom,
    *, devices, groups,
):
    number = triples_hbm.shape[1]
    needs = 3 * number
    pair_rows = surfaces.shape[0]
    mode_rows = modals_hbm.shape[0]
    modes = pair_slot_hbm.shape[0]
    capacity = needs // devices
    cap = answers.shape[1]
    slots = devices * cap
    bands = -(-mode_rows // 8)
    held_rows = 8 * bands
    spots_all = devices * held_rows
    offset = 2 * KEEP * bands
    width = moved.shape[2]
    everyone = devices * groups
    me = lax.axis_index("dev")
    group = lax.axis_index("grp")
    flat = group * devices + me

    pairs = [
        (triples_hbm, triples), (pair_slot_hbm, pair_slot), (singles_hbm, singles),
        (modals_hbm, modals), (mode_slot_hbm, mode_slot), (small_hbm, small),
        (weights_hbm, weights), (surfaces, surf),
    ]
    part = energies.shape[1] // CHUNKS
    for i in range(CHUNKS):
        span = pl.ds(i * part, part)
        pairs.append((energies.at[:, span], values.at[:, span]))
    loads = [
        pltpu.make_async_copy(source, target, load_sem.at[min(i, SMALLS + 2)]) for i, (source, target) in enumerate(pairs)
    ]
    for load in loads[:SMALLS]:
        load.start()

    barrier = pltpu.get_barrier_semaphore()

    def each_peer(action):
        def step(k, carry):
            action(lax.rem(me + k, devices))
            return carry

        lax.fori_loop(1, devices, step, 0)

    def each_other(action):
        each_peer(lambda peer: action(group, peer))
        for k in range(1, groups):
            there = lax.rem(group + k, groups)
            action(there, me)
            each_peer(lambda peer: action(there, peer))

    each_other(
        lambda there, peer: pl.semaphore_signal(barrier, inc=1, device_id=(there, peer), device_id_type=MESH)
    )
    for load in loads[SMALLS:]:
        load.start()
    for load in loads[:SMALLS]:
        load.wait()

    padded[...] = jnp.zeros_like(padded)
    padded[1, 0:modes, 0:modes] = pair_slot[...].astype(f32)
    padded[2, 0:1, 0:modes] = mode_slot[...].astype(f32)
    picks = [triples[p : p + 1, :] for p in range(3)]
    rows = iota((LANES, number), 0)
    on = [rows == pick for pick in picks]
    on_hot = [ones_at(x) for x in on]
    pair_ints = padded[1].astype(jnp.int32)
    first_two = jnp.concatenate(on_hot[:2], axis=1)
    lines = 128.0 * nn((pair_ints >> 7).astype(f32).astype(bf16), first_two)
    lines = lines + nn((pair_ints & 127).astype(f32).astype(bf16), first_two)
    chosen = [
        total(jnp.where(on[1], lines[:, :number], 0.0), 0),
        total(jnp.where(on[2], lines[:, :number], 0.0), 0),
        total(jnp.where(on[2], lines[:, number:], 0.0), 0),
    ]
    flips = [picks[0] > picks[1], picks[0] > picks[2], picks[1] > picks[2]]
    pair_ids = (jnp.concatenate(chosen, axis=1) + 0.5).astype(jnp.int32)
    holders = iota((devices, needs), 0)
    held = (pair_ids >= holders * pair_rows) & (pair_ids < (holders + 1) * pair_rows)
    held_hot = ones_at(held)
    owner = total(jnp.where(held, holders, 0), 0)
    local = pair_ids - owner * pair_rows
    before = ones_at(iota((number, number), 0) < iota((number, number), 1))
    seen = jnp.zeros((devices, 1), f32)
    ranks = []
    for p in range(3):
        block = held_hot[:, p * number : (p + 1) * number]
        mine = held[:, p * number : (p + 1) * number]
        ranks.append(total(jnp.where(mine, nn(block, before) + seen, 0.0), 0))
        seen = seen + total(jnp.where(mine, 1.0, 0.0), 1)
    rank = (jnp.concatenate(ranks, axis=1) + 0.5).astype(jnp.int32)
    place = owner * cap + rank
    at_rank = ones_at(iota((LANES, needs), 0) == rank)
    modes_hot = jnp.concatenate(on_hot, axis=1)
    slot_ids = (nn(padded[2, 0:8, :].astype(bf16), modes_hot)[0:1, :] + 0.5).astype(jnp.int32)
    homes = iota((devices, needs), 0)
    home_row = total(jnp.where(slot_ids >= (homes + 1) * mode_rows, 1, 0), 0)
    at_home = slot_ids - home_row * mode_rows
    home_hot = ones_at(homes == home_row)
    spot = home_row * held_rows + at_home
    spots = [spot[:, p * number : (p + 1) * number] for p in range(3)]
    lower, upper, third = [], [], []
    for p, (one, two, three) in enumerate(((0, 1, 2), (0, 2, 1), (1, 2, 0))):
        lower.append(jnp.where(flips[p], spots[two], spots[one]))
        upper.append(jnp.where(flips[p], spots[one], spots[two]))
        third.append(spots[three])
    told = [local >> 4, local & 15] + [jnp.concatenate(x, axis=1) for x in (lower, upper, third)]
    told = [jnp.where(held, x.astype(f32), 0.0).astype(bf16) for x in told]
    sorted_told = nt(jnp.concatenate(told, axis=0), at_rank)
    parts = [sorted_told[f * devices : (f + 1) * devices, :] for f in range(5)]
    requests = [16.0 * parts[0] + parts[1]] + parts[2:]

    modes_in[...] = jnp.zeros_like(modes_in)
    modes_in[0:mode_rows, 0 : G * S] = modals[...]
    modes_in[0:mode_rows, G * S : G * S + G] = singles[...]
    every = modes_in[:, 0 : G * S]
    spread = small[:, 0 : G * S]
    lane = iota((KEEP, G * S), 1)
    ground_weights = jnp.where((lane & (S - 1)) == 0, spread, 0.0)
    ground_here = nt(every * every, ground_weights, highest)
    single_here = nt(modes_in[:, G * S : G * S + G], small[:, G * S : G * S + G], highest)
    padded[3, 0 : modes_in.shape[0], 0:KEEP] = ground_here
    padded[3, 0 : modes_in.shape[0], KEEP : 2 * KEEP] = single_here
    base = padded[3, 0:8, :]
    for q in range(1, bands):
        base = base + pltpu.roll(padded[3, 8 * q : 8 * q + 8, :], 2 * KEEP * q, 1)
    asked = [pltpu.roll(x, offset, 1) for x in requests]
    blank = jnp.zeros((8 - len(asked), LANES), f32)
    for p in range(devices):
        message[p] = base + jnp.concatenate([x[p : p + 1, :] for x in asked] + [blank], axis=0)
    received[me] = message[me]

    pl.semaphore_wait(barrier, everyone - 1)

    def exchange(source, target, send_sem, recv_sem, there, peer):
        return pltpu.make_async_remote_copy(
            src_ref=source, dst_ref=target, send_sem=send_sem, recv_sem=recv_sem,
            device_id=(there, peer), device_id_type=MESH,
        )

    def message_copy(peer, slot, count=None):
        rows = (lambda i: i) if count is None else (lambda i: pl.ds(0, count))
        return exchange(message.at[rows(peer)], received.at[rows(slot)], send_msg, recv_msg, group, peer)

    def answer_copy(peer, slot, count=None):
        rows = (lambda i: i) if count is None else (lambda i: pl.ds(0, count))
        return exchange(answers.at[rows(peer)], arrived.at[rows(slot)], send_ans, recv_ans, group, peer)

    neighbour = lax.rem(me + 1, devices)
    all_messages = message_copy(neighbour, 0, devices - 1)
    all_answers = answer_copy(neighbour, 0, devices - 1)
    all_moments = exchange(
        moments.at[pl.ds(0, everyone - 1)], moments.at[pl.ds(0, everyone - 1)], send_mom, recv_mom, group, neighbour
    )

    each_peer(lambda peer: message_copy(peer, me).start())

    loads[SMALLS].wait()
    loads[SMALLS + 1].wait()
    w_high = weights[0:AREA, :]
    w_low = weights[AREA : 2 * AREA, :]
    table_rows = table.shape[1]
    done = 0
    while done < table_rows:
        size = min(256, table_rows - done)
        have = min(size, pair_rows - done)
        whole = have // 16 * 16
        pieces = []
        if whole:
            pieces.append(surf[done : done + whole, :])
        if size > whole:
            rest = jnp.zeros((size - whole, G * G), f32)
            if have > whole:
                tail = jnp.concatenate(
                    [surf[done + whole : done + have, :], jnp.zeros((16 - (have - whole), G * G), f32)], axis=0
                )
                pieces.append(tail)
                rest = jnp.zeros((size - whole - 16, G * G), f32)
            if rest.shape[0]:
                pieces.append(None)
        at = done
        for piece in pieces:
            if piece is None:
                table[:, at : done + size, :] = jnp.zeros((2, done + size - at, AREA), bf16)
                continue
            high, low = split(piece)
            fitted = nt(high, w_high) + nt(high, w_low) + nt(low, w_high)
            count = piece.shape[0]
            part_high, part_low = split(fitted)
            table[0, at : at + count, :] = part_high
            table[1, at : at + count, :] = part_low
            at += count
        done += size

    pltpu.make_async_copy(energies, values, load_sem.at[SMALLS + 2]).wait()

    def inner_fit(step):
        for i, j in enumerate(members(step)):
            front = values[:, j * G * G : (j + 1) * G * G]
            back = values[:, (G - 1 - j) * G * G : (G - j) * G * G]
            both = jnp.concatenate([front, back], axis=0)
            plane = nt(weights[0:AREA, :], both) + nt(weights[AREA : 2 * AREA, :], both)
            planes[step % 2, i] = plane[:, :number] + plane[:, number:]
            planes[step % 2, 4 + i] = plane[:, :number] - plane[:, number:]

    def outer_fit(step):
        for block in range(AREA // 8):
            span = slice(block * 8, block * 8 + 8)
            sums = [planes[step % 2, i, span, :] for i in range(4)]
            differences = [planes[step % 2, 4 + i, span, :] for i in range(4)]
            for c, value in enumerate(fit_orders(step, sums, differences)):
                acc[c, span, :] = value if step == 0 else acc[c, span, :] + value

    for step in range(EARLY):
        inner_fit(step)
        if step:
            outer_fit(step - 1)

    all_messages.wait_recv()
    wanted = [received[p, f : f + 1, :] for f in range(4) for p in range(devices)]
    if 4 * devices < LANES:
        wanted.append(jnp.zeros((LANES - 4 * devices, LANES), f32))
    wanted = (jnp.concatenate(wanted, axis=0).T[offset : offset + cap, :] + 0.5).astype(jnp.int32)
    in_table = iota((capacity, table_rows), 1)
    if cap > capacity:
        hits[...] = jnp.zeros_like(hits)
        modes_of[...] = jnp.zeros_like(modes_of)
    for p in range(devices):
        hits[p, 0:capacity, :] = ones_at(wanted[0:capacity, p : p + 1] == in_table)
    all_hits = hits[...].reshape(slots, table_rows)
    found = nn(all_hits, table[0]) + nn(all_hits, table[1])
    answers[...] = found.reshape(devices, cap, AREA)
    arrived[me] = answers[me]
    each_peer(lambda peer: answer_copy(peer, me).start())

    sent = received[...].reshape(devices * 8, LANES)
    for q in range(bands):
        turned = pltpu.roll(sent, LANES - 2 * KEEP * q, 1) if q else sent
        mode_table[:, 8 * q : 8 * q + 8, :] = turned.reshape(devices, 8, LANES)
    mode_rows_all = mode_table[...].reshape(spots_all, LANES)[:, 0 : 2 * KEEP]
    tables_high, tables_low = split(mode_rows_all)
    spot_hot = ones_at(iota((spots_all, needs), 0) == spot)
    taken = tn(tables_high, spot_hot) + tn(tables_low, spot_hot)
    ground = [taken[0:KEEP, p * number : (p + 1) * number] for p in range(3)]
    single = [taken[KEEP : 2 * KEEP, p * number : (p + 1) * number] for p in range(3)]

    in_spots = iota((capacity, spots_all), 1)
    for f in range(3):
        for p in range(devices):
            column = wanted[0:capacity, (f + 1) * devices + p : (f + 1) * devices + p + 1]
            hot_row = ones_at(column == in_spots)
            modes_of[f, p, 0:capacity, 0:spots_all] = hot_row
            modes_of[f, p, 0:capacity, spots_all : 2 * spots_all] = hot_row
    columns = iota((KEEP, AREA), 1)
    index = iota((KEEP, AREA), 0)
    by_first = ones_at((columns >> 4) == index)
    by_second = ones_at((columns & (KEEP - 1)) == index)
    by_zero = ones_at(index == 0)
    patterns = jnp.concatenate([by_first, by_second, by_zero], axis=1)
    wide_high, wide_low = split(nn(tables_high[:, 0:KEEP], patterns) + nn(tables_low[:, 0:KEEP], patterns))
    wide_tables = jnp.concatenate([wide_high, wide_low], axis=0)
    ground_lower, ground_upper, ground_third = [
        nn(modes_of[f].reshape(slots, 2 * spots_all), wide_tables[:, f * AREA : (f + 1) * AREA]) for f in range(3)
    ]

    def fold_orders(values, pattern):
        high, low = split(values)
        return nt(high, pattern) + nt(low, pattern)

    seen_upper = found * ground_upper
    takes = [
        fold_orders(seen_upper * ground_third, by_first),
        fold_orders(found * ground_lower * ground_third, by_second),
        fold_orders(seen_upper * ground_lower, by_zero),
    ]
    takes_high, takes_low = split(jnp.concatenate(takes, axis=0))
    asked_spots = []
    for f in range(3):
        for p in range(devices):
            asked_spots.append(received[p, f + 1 : f + 2, offset : offset + cap])
    asked_spots = jnp.concatenate(asked_spots, axis=1)
    spot_rows = (asked_spots + 0.5).astype(jnp.int32)
    turned_hot = ones_at(iota((spots_all, 3 * slots), 0) == spot_rows)
    owed = nn(turned_hot, takes_high) + nn(turned_hot, takes_low)
    owed_high, owed_low = split(owed)
    repeat = ones_at((iota((KEEP, width), 1) & (KEEP - 1)) == iota((KEEP, width), 0))
    owed = nn(owed_high, repeat) + nn(owed_low, repeat)
    wide_row = iota((spots_all, width), 0) & (held_rows - 1)
    owed_high, owed_low = split(jnp.where(wide_row == (iota((spots_all, width), 1) >> 4), owed, 0.0))
    of_home = ones_at((iota((devices, spots_all), 1) // held_rows) == iota((devices, spots_all), 0))
    owed = nn(of_home, owed_high) + nn(of_home, owed_low)

    for step in range(EARLY, STEPS):
        inner_fit(step)
        if step:
            outer_fit(step - 1)
    outer_fit(STEPS - 1)

    first_row = iota((KEEP, number), 0) == 0
    for c in range(KEEP):
        here = jnp.where(first_row, single[0][c : c + 1, :], 0.0)
        acc[c, 0:KEEP, :] -= here + single[2] if c == 0 else here
    acc[0, pl.ds(0, KEEP, stride=KEEP), :] -= single[1]
    low3, high3 = ground[2][0:8], ground[2][8:16]
    rows1 = [ground[0][c : c + 1, :] for c in range(KEEP)]
    partial1 = [jnp.zeros((8, number), f32) for _ in range(KEEP)]
    field2 = []
    field3 = [jnp.zeros((8, number), f32) for _ in range(2)]
    for d in range(KEEP):
        row2 = ground[1][d : d + 1, :]
        inner = jnp.zeros((8, number), f32)
        for h, part3 in enumerate((low3, high3)):
            weight = row2 * part3
            mixed = jnp.zeros((8, number), f32)
            for c in range(KEEP):
                value = acc[c, d * KEEP + 8 * h : d * KEEP + 8 * h + 8, :]
                partial1[c] = partial1[c] + value * weight
                mixed = mixed + value * rows1[c]
            inner = inner + mixed * part3
            field3[h] = field3[h] + mixed * row2
        field2.append(total(inner, 0))
    field1 = jnp.concatenate([total(x, 0) for x in partial1], axis=0)
    field2 = jnp.concatenate(field2, axis=0)
    field3 = jnp.concatenate(field3, axis=0)
    energy = total(field1 * ground[0], 0)

    fields = jnp.concatenate([field1, field2, field3], axis=1)
    fields = jnp.concatenate([fields] * (width // KEEP), axis=0)
    fields_high, fields_low = split(jnp.where((iota((width, needs), 0) >> 4) == at_home, fields, 0.0))
    sums = nt(home_hot, fields_high) + nt(home_hot, fields_low) - owed
    for p in range(devices):
        moved[p] = sums[p : p + 1, :]
    moments[flat] = moved[me]

    each_other(
        lambda there, peer: exchange(moved.at[peer], moments.at[flat], send_mom, recv_mom, there, peer).start()
    )

    rows16 = modes_in.shape[0]
    for g in range(G):
        exp_modals[g * rows16 : (g + 1) * rows16, 0:S] = modes_in[:, g * S : (g + 1) * S]
    pieces = exp_modals[:, 0:S]
    piece_high, piece_low = split(pieces)
    products = (nn(piece_high, by_first) + nn(piece_low, by_first)) * (nn(piece_high, by_second) + nn(piece_low, by_second))
    products_high, products_low = split(products)
    tall = jnp.concatenate([spread] * (width // KEEP), axis=0)
    own_row = (iota(tall.shape, 1) & (rows16 - 1)) == (iota(tall.shape, 0) >> 4)
    tall_high, tall_low = split(jnp.where(own_row, tall, 0.0))
    deep_high, deep_low = split(
        nn(tall_high, products_high) + nn(tall_high, products_low) + nn(tall_low, products_high)
    )
    deep[0] = deep_high
    deep[1] = deep_low

    all_answers.wait_recv()
    place_hot = ones_at(iota((slots, needs), 0) == place)
    arrived_high, arrived_low = split(arrived[...].reshape(slots, AREA))
    ordered = tn(arrived_high, place_hot) + tn(arrived_low, place_hot)
    for p in range(3):
        pair_t[p] = ordered[:, p * number : (p + 1) * number]

    def pair_rows_of(p, c):
        straight = pair_t[p, c * KEEP : (c + 1) * KEEP, :]
        turned_rows = pair_t[p, pl.ds(c, KEEP, stride=KEEP), :]
        return jnp.where(flips[p], turned_rows, straight)

    for c in range(KEEP):
        acc[c, pl.ds(0, KEEP, stride=KEEP), :] -= pair_rows_of(0, c)
        acc[c, 0:KEEP, :] -= pair_rows_of(1, c)
        acc[0, c * KEEP : (c + 1) * KEEP, :] -= pair_rows_of(2, c)

    for p, (one, two, three) in enumerate(((0, 1, 2), (0, 2, 1), (1, 2, 0))):
        ground_low = jnp.where(flips[p], ground[two], ground[one])
        ground_high = jnp.where(flips[p], ground[one], ground[two])
        share = jnp.zeros((KEEP, number), f32)
        for c in range(KEEP):
            share = share + pair_t[p, c * KEEP : (c + 1) * KEEP, :] * ground_low[c : c + 1, :]
        energy = energy - ground[three][0:1, :] * total(share * ground_high, 0)
    energy_out[...] = energy

    for c in range(KEEP):
        coefficients[:, c * AREA : (c + 1) * AREA] = acc[c].T.astype(bf16)

    all_moments.wait_recv()
    summed = moments[0]
    for k in range(1, everyone):
        summed = summed + moments[k]
    chosen_rows = (iota((rows16, width), 1) >> 4) == iota((rows16, width), 0)
    mean_high, mean_low = split(jnp.where(chosen_rows, summed, 0.0))
    mean = nn(mean_high, deep[0]) + nn(mean_high, deep[1]) + nn(mean_low, deep[0])
    mean_out[...] = mean[0:mode_rows, :]

    all_messages.wait_send()
    all_answers.wait_send()
    all_moments.wait_send()


def write_kernel(coefficients, energy, mean, coefficients_out, energy_out, mean_out, sems):
    copies = [
        pltpu.make_async_copy(source, target, sems.at[i])
        for i, (source, target) in enumerate(
            [(coefficients, coefficients_out), (energy, energy_out), (mean, mean_out)]
        )
    ]
    for copy in copies:
        copy.start()
    for copy in copies:
        copy.wait()


def body(energies, triples, pair_surfaces, pair_slot, single_surfaces, modals, mode_slot):
    devices = lax.axis_size("dev")
    groups = lax.axis_size("grp")
    number = triples.shape[0]
    pair_rows = pair_surfaces.shape[0]
    mode_rows = modals.shape[0]
    cap = round_up(3 * number // devices, 16)
    table_rows = round_up(pair_rows, 256)
    width = round_up(mode_rows * KEEP, LANES)
    rows16 = 16
    held_rows = round_up(mode_rows, 8)
    spots_all = devices * held_rows
    everyone = devices * groups
    vmem = pl.BlockSpec(memory_space=pltpu.VMEM)
    hbm = pl.BlockSpec(memory_space=pltpu.HBM)
    small_shapes = [
        (triples.shape[::-1], jnp.int32), (pair_slot.shape, jnp.int32), (single_surfaces.shape, f32),
        (modals.shape, f32), ((1, mode_slot.shape[0]), jnp.int32), (SMALL.shape, f32),
    ]
    results = [
        jax.ShapeDtypeStruct((number, KEEP * AREA), bf16),
        jax.ShapeDtypeStruct((1, number), f32),
        jax.ShapeDtypeStruct((mode_rows, S * S), f32),
    ]
    in_vmem = pl.pallas_call(
        functools.partial(kernel, devices=devices, groups=groups),
        in_specs=[hbm] * 9,
        out_specs=[vmem, vmem, vmem],
        out_shape=results,
        scratch_shapes=[
            *[pltpu.VMEM(shape, kind) for shape, kind in small_shapes],
            pltpu.VMEM(energies.shape, bf16),
            pltpu.VMEM(pair_surfaces.shape, f32),
            pltpu.VMEM(WEIGHTS.shape, bf16),
            pltpu.VMEM((2, 8, AREA, number), f32),
            pltpu.VMEM((KEEP, AREA, number), f32),
            pltpu.VMEM((2, table_rows, AREA), bf16),
            pltpu.VMEM((devices, cap, table_rows), bf16),
            pltpu.VMEM((devices, cap, AREA), f32),
            pltpu.VMEM((devices, cap, AREA), f32),
            pltpu.VMEM((3, AREA, number), f32),
            pltpu.VMEM((4, LANES, LANES), f32),
            pltpu.VMEM((devices, 8, LANES), f32),
            pltpu.VMEM((devices, 8, LANES), f32),
            pltpu.VMEM((3, devices, cap, 2 * spots_all), bf16),
            pltpu.VMEM((devices, held_rows, LANES), f32),
            pltpu.VMEM((rows16, SMALL.shape[1]), f32),
            pltpu.VMEM((G * rows16, LANES), f32),
            pltpu.VMEM((2, width, AREA), bf16),
            pltpu.VMEM((devices, 1, width), f32),
            pltpu.VMEM((everyone, 1, width), f32),
            pltpu.SemaphoreType.DMA((SMALLS + 3,)),
            *[pltpu.SemaphoreType.DMA] * 6,
        ],
        compiler_params=pltpu.CompilerParams(
            collective_id=0, has_side_effects=True, vmem_limit_bytes=32 * 1024 * 1024
        ),
    )(
        *[
            pltpu.with_memory_space_constraint(x, pltpu.HBM)
            for x in (
                energies, triples.T, pair_surfaces, pair_slot, single_surfaces, modals, mode_slot.reshape(1, -1),
                jnp.asarray(WEIGHTS), jnp.asarray(SMALL),
            )
        ]
    )
    coefficients, energy, mean = pl.pallas_call(
        write_kernel,
        in_specs=[vmem] * 3,
        out_specs=[hbm] * 3,
        out_shape=results,
        scratch_shapes=[pltpu.SemaphoreType.DMA((3,))],
        compiler_params=pltpu.CompilerParams(vmem_limit_bytes=1024 * 1024),
    )(*in_vmem)
    return coefficients, energy.reshape(number), mean


def solution(mesh):
    in_specs = (
        P(("grp", "dev"), None),
        P(("grp", "dev"), None),
        P("dev", None),
        P(),
        P("dev", None),
        P("dev", None),
        P(),
    )
    out_specs = (P(("grp", "dev"), None), P(("grp", "dev")), P("dev", None))
    return jax.shard_map(body, mesh=mesh, in_specs=in_specs, out_specs=out_specs, check_vma=False)
```

```python
import functools

import jax
import jax.numpy as jnp
import numpy as np
from jax import lax
from jax.experimental import pallas as pl
from jax.experimental.pallas import tpu as pltpu
from jax.sharding import PartitionSpec as P

G = 32
KEEP = 16
S = 16
AREA = KEEP * KEEP
HALF = G // 2
LANES = 128
STEPS = 4
EARLY = 1
CHUNKS = 8
SMALLS = 6
UNROLLED = 8
MESH = pl.DeviceIdType.MESH
f32 = jnp.float32
bf16 = jnp.bfloat16
highest = lax.Precision.HIGHEST


def np_tables():
    orders = np.arange(KEEP, dtype=np.float64)
    points = np.arange(G, dtype=np.float64) + 0.5
    cosines = np.cos(np.pi * orders[:, None] * points[None, :] / G)
    weights = np.where(orders == 0, 1.0, 2.0) / G
    return cosines, weights[:, None] * cosines


COS, FIT = np_tables()


def split_np(values):
    values = np.asarray(values, np.float32)
    high = values.astype(jnp.bfloat16)
    return high, (values - high.astype(np.float32)).astype(jnp.bfloat16)


INNER = np.einsum("dh,el->dehl", FIT, FIT).reshape(AREA, G * G)
WEIGHTS = np.concatenate(split_np(INNER), axis=0)
ACROSS = np.concatenate(split_np(INNER.T), axis=1)
SMALL = np.concatenate([np.repeat(COS, S, axis=1), FIT, np.zeros((KEEP, LANES - G))], axis=1).astype(np.float32)


def round_up(value, step):
    return -(-value // step) * step


def iota(shape, axis):
    return lax.broadcasted_iota(jnp.int32, shape, axis)


def nn(a, b, precision=None):
    return lax.dot_general(a, b, (((1,), (0,)), ((), ())), precision=precision, preferred_element_type=f32)


def nt(a, b, precision=None):
    return lax.dot_general(a, b, (((1,), (1,)), ((), ())), precision=precision, preferred_element_type=f32)


def tn(a, b, precision=None):
    return lax.dot_general(a, b, (((0,), (0,)), ((), ())), precision=precision, preferred_element_type=f32)


def split(values):
    high = values.astype(bf16)
    return high, (values - high.astype(f32)).astype(bf16)


def ones_at(mask):
    return jnp.where(mask, 1.0, 0.0).astype(bf16)


def total(values, axis):
    return jnp.sum(values, axis=axis, keepdims=True)


def members(step):
    return step, 15 - step, 7 - step, 8 + step


def fit_orders(step, s, d):
    js = members(step)
    u, v = (s[0] + s[1], s[2] + s[3]), (s[0] - s[1], s[2] - s[3])
    out = []
    for c in range(KEEP):
        if c % 2:
            terms = list(zip(js, d))
        elif c % 4:
            terms = [(js[0], v[0]), (js[2], v[1])]
        elif c % 8:
            terms = [(js[0], u[0] - u[1])]
        else:
            terms = [(js[0], u[0] + u[1])]
        value = None
        for j, term in terms:
            scaled = float(FIT[c, j]) * term
            value = scaled if value is None else value + scaled
        out.append(value)
    return out


def kernel(
    energies, triples_hbm, surfaces, pair_slot_hbm, singles_hbm, modals_hbm, mode_slot_hbm, across_hbm, weights_hbm, small_hbm,
    coefficients, energy_out, mean_out,
    triples, pair_slot, singles, modals, mode_slot, small,
    values, surf, across, weights, planes, acc, table, answers, arrived, pair_t, padded, message, received,
    modes_of, mode_table, modes_in, exp_modals, deep, moved, moments,
    load_sem, send_msg, recv_msg, send_ans, recv_ans, send_mom, recv_mom,
    *, devices, groups,
):
    number = triples_hbm.shape[1]
    needs = 3 * number
    pair_rows = surfaces.shape[0]
    mode_rows = modals_hbm.shape[0]
    modes = pair_slot_hbm.shape[0]
    capacity = needs // devices
    cap = answers.shape[1]
    slots = devices * cap
    bands = -(-mode_rows // 8)
    held_rows = 8 * bands
    spots_all = devices * held_rows
    offset = 2 * KEEP * bands
    width = moved.shape[2]
    everyone = devices * groups
    me = lax.axis_index("dev")
    group = lax.axis_index("grp")
    flat = group * devices + me

    pairs = [
        (triples_hbm, triples), (pair_slot_hbm, pair_slot), (singles_hbm, singles),
        (modals_hbm, modals), (mode_slot_hbm, mode_slot), (small_hbm, small),
        (across_hbm, across), (surfaces, surf), (weights_hbm, weights),
    ]
    part = energies.shape[1] // CHUNKS
    for i in range(CHUNKS):
        span = pl.ds(i * part, part)
        pairs.append((energies.at[:, span], values.at[:, span]))
    loads = [
        pltpu.make_async_copy(source, target, load_sem.at[min(i, SMALLS + 3)]) for i, (source, target) in enumerate(pairs)
    ]
    barrier = pltpu.get_barrier_semaphore()

    def after(position, k, size):
        moved_on = position + k
        return jnp.where(moved_on >= size, moved_on - size, moved_on)

    def each_peer(action):
        if devices <= UNROLLED:
            for k in range(1, devices):
                action(after(me, k, devices))
            return

        def step(k, carry):
            action(after(me, k, devices))
            return carry

        lax.fori_loop(1, devices, step, 0)

    def each_other(action):
        each_peer(lambda peer: action(group, peer))
        for k in range(1, groups):
            there = after(group, k, groups)
            action(there, me)
            each_peer(lambda peer: action(there, peer))

    each_other(
        lambda there, peer: pl.semaphore_signal(barrier, inc=1, device_id=(there, peer), device_id_type=MESH)
    )
    for load in loads[: SMALLS + 2]:
        load.start()
    for load in loads[:SMALLS]:
        load.wait()

    padded[...] = jnp.zeros_like(padded)
    padded[1, 0:modes, 0:modes] = pair_slot[...].astype(f32)
    padded[2, 0:1, 0:modes] = mode_slot[...].astype(f32)
    picks = [triples[p : p + 1, :] for p in range(3)]
    rows = iota((LANES, number), 0)
    on = [rows == pick for pick in picks]
    on_hot = [ones_at(x) for x in on]
    pair_ints = padded[1].astype(jnp.int32)
    first_two = jnp.concatenate(on_hot[:2], axis=1)
    lines = 128.0 * nn((pair_ints >> 7).astype(f32).astype(bf16), first_two)
    lines = lines + nn((pair_ints & 127).astype(f32).astype(bf16), first_two)
    chosen = [
        total(jnp.where(on[1], lines[:, :number], 0.0), 0),
        total(jnp.where(on[2], lines[:, :number], 0.0), 0),
        total(jnp.where(on[2], lines[:, number:], 0.0), 0),
    ]
    flips = [picks[0] > picks[1], picks[0] > picks[2], picks[1] > picks[2]]
    pair_ids = (jnp.concatenate(chosen, axis=1) + 0.5).astype(jnp.int32)
    holders = iota((devices, needs), 0)
    held = (pair_ids >= holders * pair_rows) & (pair_ids < (holders + 1) * pair_rows)
    held_hot = ones_at(held)
    owner = total(jnp.where(held, holders, 0), 0)
    local = pair_ids - owner * pair_rows
    before = ones_at(iota((number, number), 0) < iota((number, number), 1))
    seen = jnp.zeros((devices, 1), f32)
    ranks = []
    for p in range(3):
        block = held_hot[:, p * number : (p + 1) * number]
        mine = held[:, p * number : (p + 1) * number]
        ranks.append(total(jnp.where(mine, nn(block, before) + seen, 0.0), 0))
        seen = seen + total(jnp.where(mine, 1.0, 0.0), 1)
    rank = (jnp.concatenate(ranks, axis=1) + 0.5).astype(jnp.int32)
    place = owner * cap + rank
    at_rank = ones_at(iota((LANES, needs), 0) == rank)
    modes_hot = jnp.concatenate(on_hot, axis=1)
    slot_ids = (nn(padded[2, 0:8, :].astype(bf16), modes_hot)[0:1, :] + 0.5).astype(jnp.int32)
    homes = iota((devices, needs), 0)
    home_row = total(jnp.where(slot_ids >= (homes + 1) * mode_rows, 1, 0), 0)
    at_home = slot_ids - home_row * mode_rows
    home_hot = ones_at(homes == home_row)
    spot = home_row * held_rows + at_home
    spots = [spot[:, p * number : (p + 1) * number] for p in range(3)]
    lower, upper, third = [], [], []
    for p, (one, two, three) in enumerate(((0, 1, 2), (0, 2, 1), (1, 2, 0))):
        lower.append(jnp.where(flips[p], spots[two], spots[one]))
        upper.append(jnp.where(flips[p], spots[one], spots[two]))
        third.append(spots[three])
    told = [local >> 4, local & 15] + [jnp.concatenate(x, axis=1) for x in (lower, upper, third)]
    told = [jnp.where(held, x.astype(f32), 0.0).astype(bf16) for x in told]
    sorted_told = nt(jnp.concatenate(told, axis=0), at_rank)
    parts = [sorted_told[f * devices : (f + 1) * devices, :] for f in range(5)]
    requests = [16.0 * parts[0] + parts[1]] + parts[2:]

    modes_in[...] = jnp.zeros_like(modes_in)
    modes_in[0:mode_rows, 0 : G * S] = modals[...]
    modes_in[0:mode_rows, G * S : G * S + G] = singles[...]
    every = modes_in[:, 0 : G * S]
    spread = small[:, 0 : G * S]
    lane = iota((KEEP, G * S), 1)
    ground_weights = jnp.where((lane & (S - 1)) == 0, spread, 0.0)
    ground_here = nt(every * every, ground_weights, highest)
    single_here = nt(modes_in[:, G * S : G * S + G], small[:, G * S : G * S + G], highest)
    padded[3, 0 : modes_in.shape[0], 0:KEEP] = ground_here
    padded[3, 0 : modes_in.shape[0], KEEP : 2 * KEEP] = single_here
    base = padded[3, 0:8, :]
    for q in range(1, bands):
        base = base + pltpu.roll(padded[3, 8 * q : 8 * q + 8, :], 2 * KEEP * q, 1)
    asked = [pltpu.roll(x, offset, 1) for x in requests]
    blank = jnp.zeros((8 - len(asked), LANES), f32)
    for p in range(devices):
        message[p] = base + jnp.concatenate([x[p : p + 1, :] for x in asked] + [blank], axis=0)
    received[me] = message[me]

    for load in loads[SMALLS + 2 :]:
        load.start()
    pl.semaphore_wait(barrier, everyone - 1)

    def exchange(source, target, send_sem, recv_sem, there, peer):
        return pltpu.make_async_remote_copy(
            src_ref=source, dst_ref=target, send_sem=send_sem, recv_sem=recv_sem,
            device_id=(there, peer), device_id_type=MESH,
        )

    def message_copy(peer, slot, count=None):
        rows = (lambda i: i) if count is None else (lambda i: pl.ds(0, count))
        return exchange(message.at[rows(peer)], received.at[rows(slot)], send_msg, recv_msg, group, peer)

    def answer_copy(peer, slot, count=None):
        rows = (lambda i: i) if count is None else (lambda i: pl.ds(0, count))
        return exchange(answers.at[rows(peer)], arrived.at[rows(slot)], send_ans, recv_ans, group, peer)

    neighbour = lax.rem(me + 1, devices)
    all_messages = message_copy(neighbour, 0, devices - 1)
    all_answers = answer_copy(neighbour, 0, devices - 1)
    all_moments = exchange(
        moments.at[pl.ds(0, everyone - 1)], moments.at[pl.ds(0, everyone - 1)], send_mom, recv_mom, group, neighbour
    )

    each_peer(lambda peer: message_copy(peer, me).start())

    loads[SMALLS].wait()
    loads[SMALLS + 1].wait()
    table_rows = table.shape[1]
    done = 0
    while done < table_rows:
        size = min(256, table_rows - done)
        have = min(size, pair_rows - done)
        whole = have // 16 * 16
        pieces = []
        if whole:
            pieces.append(surf[done : done + whole, :])
        if size > whole:
            rest = jnp.zeros((size - whole, G * G), f32)
            if have > whole:
                tail = jnp.concatenate(
                    [surf[done + whole : done + have, :], jnp.zeros((16 - (have - whole), G * G), f32)], axis=0
                )
                pieces.append(tail)
                rest = jnp.zeros((size - whole - 16, G * G), f32)
            if rest.shape[0]:
                pieces.append(None)
        at = done
        for piece in pieces:
            if piece is None:
                table[:, at : done + size, :] = jnp.zeros((2, done + size - at, AREA), bf16)
                continue
            high, low = split(piece)
            both_parts = nn(high, across[...])
            fitted = both_parts[:, 0:AREA] + both_parts[:, AREA : 2 * AREA] + nn(low, across[:, 0:AREA])
            count = piece.shape[0]
            part_high, part_low = split(fitted)
            table[0, at : at + count, :] = part_high
            table[1, at : at + count, :] = part_low
            at += count
        done += size

    loads[SMALLS + 2].wait()
    pltpu.make_async_copy(energies, values, load_sem.at[SMALLS + 3]).wait()

    def inner_fit(step):
        for i, j in enumerate(members(step)):
            front = values[:, j * G * G : (j + 1) * G * G]
            back = values[:, (G - 1 - j) * G * G : (G - j) * G * G]
            both = jnp.concatenate([front, back], axis=0)
            plane = nt(weights[0:AREA, :], both) + nt(weights[AREA : 2 * AREA, :], both)
            planes[step % 2, i] = plane[:, :number] + plane[:, number:]
            planes[step % 2, 4 + i] = plane[:, :number] - plane[:, number:]

    def outer_fit(step):
        for block in range(AREA // 8):
            span = slice(block * 8, block * 8 + 8)
            sums = [planes[step % 2, i, span, :] for i in range(4)]
            differences = [planes[step % 2, 4 + i, span, :] for i in range(4)]
            for c, value in enumerate(fit_orders(step, sums, differences)):
                acc[c, span, :] = value if step == 0 else acc[c, span, :] + value

    for step in range(EARLY):
        inner_fit(step)
        if step:
            outer_fit(step - 1)

    all_messages.wait_recv()
    wanted = [received[p, f : f + 1, :] for f in range(4) for p in range(devices)]
    if 4 * devices < LANES:
        wanted.append(jnp.zeros((LANES - 4 * devices, LANES), f32))
    wanted = (jnp.concatenate(wanted, axis=0).T[offset : offset + cap, :] + 0.5).astype(jnp.int32)
    in_table = iota((cap, table_rows), 1)
    if cap > capacity:
        modes_of[...] = jnp.zeros_like(modes_of)
    found = []
    half = max(1, devices // 2)
    for start in range(0, devices, half):
        rows_hot = jnp.concatenate(
            [ones_at(wanted[:, p : p + 1] == in_table) for p in range(start, start + half)], axis=0
        )
        found.append(nn(rows_hot, table[0]) + nn(rows_hot, table[1]))
        answers[start : start + half] = found[-1].reshape(half, cap, AREA)
    found = jnp.concatenate(found, axis=0)
    arrived[me] = answers[me]
    each_peer(lambda peer: answer_copy(peer, me).start())

    sent = received[...].reshape(devices * 8, LANES)
    for q in range(bands):
        turned = pltpu.roll(sent, LANES - 2 * KEEP * q, 1) if q else sent
        mode_table[:, 8 * q : 8 * q + 8, :] = turned.reshape(devices, 8, LANES)
    mode_rows_all = mode_table[...].reshape(spots_all, LANES)[:, 0 : 2 * KEEP]
    tables_high, tables_low = split(mode_rows_all)
    spot_hot = ones_at(iota((spots_all, needs), 0) == spot)
    taken = tn(tables_high, spot_hot) + tn(tables_low, spot_hot)
    ground = [taken[0:KEEP, p * number : (p + 1) * number] for p in range(3)]
    single = [taken[KEEP : 2 * KEEP, p * number : (p + 1) * number] for p in range(3)]

    in_spots = iota((capacity, spots_all), 1)
    for f in range(3):
        for p in range(devices):
            column = wanted[0:capacity, (f + 1) * devices + p : (f + 1) * devices + p + 1]
            hot_row = ones_at(column == in_spots)
            modes_of[f, p, 0:capacity, 0:spots_all] = hot_row
            modes_of[f, p, 0:capacity, spots_all : 2 * spots_all] = hot_row
    columns = iota((KEEP, AREA), 1)
    index = iota((KEEP, AREA), 0)
    by_first = ones_at((columns >> 4) == index)
    by_second = ones_at((columns & (KEEP - 1)) == index)
    by_zero = ones_at(index == 0)
    patterns = jnp.concatenate([by_first, by_second, by_zero], axis=1)
    wide_high, wide_low = split(nn(tables_high[:, 0:KEEP], patterns) + nn(tables_low[:, 0:KEEP], patterns))
    wide_tables = jnp.concatenate([wide_high, wide_low], axis=0)
    def fold_orders(values, pattern):
        high, low = split(values)
        return nt(high, pattern) + nt(low, pattern)

    def fit_step(step):
        if step < STEPS:
            inner_fit(step)
        if step:
            outer_fit(step - 1)

    ground_lower, ground_upper, ground_third = [
        nn(modes_of[f].reshape(slots, 2 * spots_all), wide_tables[:, f * AREA : (f + 1) * AREA]) for f in range(3)
    ]

    fit_step(EARLY)

    seen_upper = found * ground_upper
    takes = [
        fold_orders(seen_upper * ground_third, by_first),
        fold_orders(found * ground_lower * ground_third, by_second),
        fold_orders(seen_upper * ground_lower, by_zero),
    ]
    fit_step(EARLY + 1)

    takes_high, takes_low = split(jnp.concatenate(takes, axis=0))
    asked_spots = []
    for f in range(3):
        for p in range(devices):
            asked_spots.append(received[p, f + 1 : f + 2, offset : offset + cap])
    asked_spots = jnp.concatenate(asked_spots, axis=1)
    spot_rows = (asked_spots + 0.5).astype(jnp.int32)
    turned_hot = ones_at(iota((spots_all, 3 * slots), 0) == spot_rows)
    owed = nn(turned_hot, takes_high) + nn(turned_hot, takes_low)
    owed_high, owed_low = split(owed)
    repeat = ones_at((iota((KEEP, width), 1) & (KEEP - 1)) == iota((KEEP, width), 0))
    owed = nn(owed_high, repeat) + nn(owed_low, repeat)
    wide_row = iota((spots_all, width), 0) & (held_rows - 1)
    owed_high, owed_low = split(jnp.where(wide_row == (iota((spots_all, width), 1) >> 4), owed, 0.0))
    of_home = ones_at((iota((devices, spots_all), 1) // held_rows) == iota((devices, spots_all), 0))
    owed = nn(of_home, owed_high) + nn(of_home, owed_low)
    for step in range(EARLY + 2, STEPS + 1):
        fit_step(step)

    first_row = iota((KEEP, number), 0) == 0
    for c in range(KEEP):
        here = jnp.where(first_row, single[0][c : c + 1, :], 0.0)
        acc[c, 0:KEEP, :] -= here + single[2] if c == 0 else here
    acc[0, pl.ds(0, KEEP, stride=KEEP), :] -= single[1]
    low3, high3 = ground[2][0:8], ground[2][8:16]
    rows1 = [ground[0][c : c + 1, :] for c in range(KEEP)]
    partial1 = [jnp.zeros((8, number), f32) for _ in range(KEEP)]
    field2 = []
    field3 = [jnp.zeros((8, number), f32) for _ in range(2)]
    for d in range(KEEP):
        row2 = ground[1][d : d + 1, :]
        inner = jnp.zeros((8, number), f32)
        for h, part3 in enumerate((low3, high3)):
            weight = row2 * part3
            mixed = jnp.zeros((8, number), f32)
            for c in range(KEEP):
                value = acc[c, d * KEEP + 8 * h : d * KEEP + 8 * h + 8, :]
                partial1[c] = partial1[c] + value * weight
                mixed = mixed + value * rows1[c]
            inner = inner + mixed * part3
            field3[h] = field3[h] + mixed * row2
        field2.append(total(inner, 0))
    field1 = jnp.concatenate([total(x, 0) for x in partial1], axis=0)
    field2 = jnp.concatenate(field2, axis=0)
    field3 = jnp.concatenate(field3, axis=0)
    energy = total(field1 * ground[0], 0)

    fields = jnp.concatenate([field1, field2, field3], axis=1)
    fields = jnp.concatenate([fields] * (width // KEEP), axis=0)
    fields_high, fields_low = split(jnp.where((iota((width, needs), 0) >> 4) == at_home, fields, 0.0))
    sums = nt(home_hot, fields_high) + nt(home_hot, fields_low) - owed
    for p in range(devices):
        moved[p] = sums[p : p + 1, :]
    moments[flat] = moved[me]

    each_other(
        lambda there, peer: exchange(moved.at[peer], moments.at[flat], send_mom, recv_mom, there, peer).start()
    )

    rows16 = modes_in.shape[0]
    for g in range(G):
        exp_modals[g * rows16 : (g + 1) * rows16, 0:S] = modes_in[:, g * S : (g + 1) * S]
    pieces = exp_modals[:, 0:S]
    piece_high, piece_low = split(pieces)
    products = (nn(piece_high, by_first) + nn(piece_low, by_first)) * (nn(piece_high, by_second) + nn(piece_low, by_second))
    products_high, products_low = split(products)
    tall = jnp.concatenate([spread] * (width // KEEP), axis=0)
    own_row = (iota(tall.shape, 1) & (rows16 - 1)) == (iota(tall.shape, 0) >> 4)
    tall_high, tall_low = split(jnp.where(own_row, tall, 0.0))
    deep_high, deep_low = split(
        nn(tall_high, products_high) + nn(tall_high, products_low) + nn(tall_low, products_high)
    )
    deep[0] = deep_high
    deep[1] = deep_low

    all_answers.wait_recv()
    place_hot = ones_at(iota((slots, needs), 0) == place)
    arrived_high, arrived_low = split(arrived[...].reshape(slots, AREA))
    ordered = tn(arrived_high, place_hot) + tn(arrived_low, place_hot)
    for p in range(3):
        pair_t[p] = ordered[:, p * number : (p + 1) * number]

    def pair_rows_of(p, c):
        straight = pair_t[p, c * KEEP : (c + 1) * KEEP, :]
        turned_rows = pair_t[p, pl.ds(c, KEEP, stride=KEEP), :]
        return jnp.where(flips[p], turned_rows, straight)

    for c in range(KEEP):
        acc[c, pl.ds(0, KEEP, stride=KEEP), :] -= pair_rows_of(0, c)
        acc[c, 0:KEEP, :] -= pair_rows_of(1, c)
        acc[0, c * KEEP : (c + 1) * KEEP, :] -= pair_rows_of(2, c)

    for p, (one, two, three) in enumerate(((0, 1, 2), (0, 2, 1), (1, 2, 0))):
        ground_low = jnp.where(flips[p], ground[two], ground[one])
        ground_high = jnp.where(flips[p], ground[one], ground[two])
        share = jnp.zeros((KEEP, number), f32)
        for c in range(KEEP):
            share = share + pair_t[p, c * KEEP : (c + 1) * KEEP, :] * ground_low[c : c + 1, :]
        energy = energy - ground[three][0:1, :] * total(share * ground_high, 0)
    energy_out[...] = energy

    for c in range(KEEP):
        coefficients[:, c * AREA : (c + 1) * AREA] = acc[c].T.astype(bf16)

    all_moments.wait_recv()
    summed = moments[0]
    for k in range(1, everyone):
        summed = summed + moments[k]
    chosen_rows = (iota((rows16, width), 1) >> 4) == iota((rows16, width), 0)
    mean_high, mean_low = split(jnp.where(chosen_rows, summed, 0.0))
    mean = nn(mean_high, deep[0]) + nn(mean_high, deep[1]) + nn(mean_low, deep[0])
    mean_out[...] = mean[0:mode_rows, :]

    all_messages.wait_send()
    all_answers.wait_send()
    all_moments.wait_send()


def write_kernel(coefficients, energy, mean, coefficients_out, energy_out, mean_out, sems):
    copies = [
        pltpu.make_async_copy(source, target, sems.at[i])
        for i, (source, target) in enumerate(
            [(coefficients, coefficients_out), (energy, energy_out), (mean, mean_out)]
        )
    ]
    for copy in copies:
        copy.start()
    for copy in copies:
        copy.wait()


def body(energies, triples, pair_surfaces, pair_slot, single_surfaces, modals, mode_slot):
    devices = lax.axis_size("dev")
    groups = lax.axis_size("grp")
    number = triples.shape[0]
    pair_rows = pair_surfaces.shape[0]
    mode_rows = modals.shape[0]
    cap = round_up(3 * number // devices, 16)
    table_rows = round_up(pair_rows, 256)
    width = round_up(mode_rows * KEEP, LANES)
    rows16 = 16
    held_rows = round_up(mode_rows, 8)
    spots_all = devices * held_rows
    everyone = devices * groups
    vmem = pl.BlockSpec(memory_space=pltpu.VMEM)
    hbm = pl.BlockSpec(memory_space=pltpu.HBM)
    small_shapes = [
        (triples.shape[::-1], jnp.int32), (pair_slot.shape, jnp.int32), (single_surfaces.shape, f32),
        (modals.shape, f32), ((1, mode_slot.shape[0]), jnp.int32), (SMALL.shape, f32),
    ]
    results = [
        jax.ShapeDtypeStruct((number, KEEP * AREA), bf16),
        jax.ShapeDtypeStruct((1, number), f32),
        jax.ShapeDtypeStruct((mode_rows, S * S), f32),
    ]
    in_vmem = pl.pallas_call(
        functools.partial(kernel, devices=devices, groups=groups),
        in_specs=[hbm] * 10,
        out_specs=[vmem, vmem, vmem],
        out_shape=results,
        scratch_shapes=[
            *[pltpu.VMEM(shape, kind) for shape, kind in small_shapes],
            pltpu.VMEM(energies.shape, bf16),
            pltpu.VMEM(pair_surfaces.shape, f32),
            pltpu.VMEM(ACROSS.shape, bf16),
            pltpu.VMEM(WEIGHTS.shape, bf16),
            pltpu.VMEM((2, 8, AREA, number), f32),
            pltpu.VMEM((KEEP, AREA, number), f32),
            pltpu.VMEM((2, table_rows, AREA), bf16),
            pltpu.VMEM((devices, cap, AREA), f32),
            pltpu.VMEM((devices, cap, AREA), f32),
            pltpu.VMEM((3, AREA, number), f32),
            pltpu.VMEM((4, LANES, LANES), f32),
            pltpu.VMEM((devices, 8, LANES), f32),
            pltpu.VMEM((devices, 8, LANES), f32),
            pltpu.VMEM((3, devices, cap, 2 * spots_all), bf16),
            pltpu.VMEM((devices, held_rows, LANES), f32),
            pltpu.VMEM((rows16, SMALL.shape[1]), f32),
            pltpu.VMEM((G * rows16, LANES), f32),
            pltpu.VMEM((2, width, AREA), bf16),
            pltpu.VMEM((devices, 1, width), f32),
            pltpu.VMEM((everyone, 1, width), f32),
            pltpu.SemaphoreType.DMA((SMALLS + 4,)),
            *[pltpu.SemaphoreType.DMA] * 6,
        ],
        compiler_params=pltpu.CompilerParams(
            collective_id=0, has_side_effects=True, vmem_limit_bytes=32 * 1024 * 1024
        ),
    )(
        *[
            pltpu.with_memory_space_constraint(x, pltpu.HBM)
            for x in (
                energies, triples.T, pair_surfaces, pair_slot, single_surfaces, modals, mode_slot.reshape(1, -1),
                jnp.asarray(ACROSS), jnp.asarray(WEIGHTS), jnp.asarray(SMALL),
            )
        ]
    )
    coefficients, energy, mean = pl.pallas_call(
        write_kernel,
        in_specs=[vmem] * 3,
        out_specs=[hbm] * 3,
        out_shape=results,
        scratch_shapes=[pltpu.SemaphoreType.DMA((3,))],
        compiler_params=pltpu.CompilerParams(vmem_limit_bytes=1024 * 1024),
    )(*in_vmem)
    return coefficients, energy.reshape(number), mean


def solution(mesh):
    in_specs = (
        P(("grp", "dev"), None),
        P(("grp", "dev"), None),
        P("dev", None),
        P(),
        P("dev", None),
        P("dev", None),
        P(),
    )
    out_specs = (P(("grp", "dev"), None), P(("grp", "dev")), P("dev", None))
    return jax.shard_map(body, mesh=mesh, in_specs=in_specs, out_specs=out_specs, check_vma=False)
```

```python
import functools

import jax
import jax.numpy as jnp
import numpy as np
from jax import lax
from jax.experimental import pallas as pl
from jax.experimental.pallas import tpu as pltpu
from jax.sharding import PartitionSpec as P

G = 32
KEEP = 16
S = 16
AREA = KEEP * KEEP
HALF = G // 2
LANES = 128
STEPS = 4
EARLY = 1
CHUNKS = 8
SMALLS = 6
UNROLLED = 8
MESH = pl.DeviceIdType.MESH
f32 = jnp.float32
bf16 = jnp.bfloat16
highest = lax.Precision.HIGHEST


def np_tables():
    orders = np.arange(KEEP, dtype=np.float64)
    points = np.arange(G, dtype=np.float64) + 0.5
    cosines = np.cos(np.pi * orders[:, None] * points[None, :] / G)
    weights = np.where(orders == 0, 1.0, 2.0) / G
    return cosines, weights[:, None] * cosines


COS, FIT = np_tables()


def split_np(values):
    values = np.asarray(values, np.float32)
    high = values.astype(jnp.bfloat16)
    return high, (values - high.astype(np.float32)).astype(jnp.bfloat16)


INNER = np.einsum("dh,el->hlde", FIT, FIT).reshape(G * G, AREA)
ACROSS = np.concatenate(split_np(INNER), axis=1)
SMALL = np.concatenate([np.repeat(COS, S, axis=1), FIT, np.zeros((KEEP, LANES - G))], axis=1).astype(np.float32)


def round_up(value, step):
    return -(-value // step) * step


def iota(shape, axis):
    return lax.broadcasted_iota(jnp.int32, shape, axis)


def nn(a, b, precision=None):
    return lax.dot_general(a, b, (((1,), (0,)), ((), ())), precision=precision, preferred_element_type=f32)


def nt(a, b, precision=None):
    return lax.dot_general(a, b, (((1,), (1,)), ((), ())), precision=precision, preferred_element_type=f32)


def tn(a, b, precision=None):
    return lax.dot_general(a, b, (((0,), (0,)), ((), ())), precision=precision, preferred_element_type=f32)


def split(values):
    high = values.astype(bf16)
    return high, (values - high.astype(f32)).astype(bf16)


def ones_at(mask):
    return jnp.where(mask, 1.0, 0.0).astype(bf16)


def total(values, axis):
    return jnp.sum(values, axis=axis, keepdims=True)


def members(step):
    return step, 15 - step, 7 - step, 8 + step


def fit_orders(step, s, d):
    js = members(step)
    u, v = (s[0] + s[1], s[2] + s[3]), (s[0] - s[1], s[2] - s[3])
    out = []
    for c in range(KEEP):
        if c % 2:
            terms = list(zip(js, d))
        elif c % 4:
            terms = [(js[0], v[0]), (js[2], v[1])]
        elif c % 8:
            terms = [(js[0], u[0] - u[1])]
        else:
            terms = [(js[0], u[0] + u[1])]
        value = None
        for j, term in terms:
            scaled = float(FIT[c, j]) * term
            value = scaled if value is None else value + scaled
        out.append(value)
    return out


def kernel(
    energies, triples_hbm, surfaces, pair_slot_hbm, singles_hbm, modals_hbm, mode_slot_hbm, across_hbm, small_hbm,
    coefficients, energy_out, mean_out,
    triples, pair_slot, singles, modals, mode_slot, small,
    values, surf, across, planes, acc, table, answers, arrived, pair_t, padded, message, received,
    modes_of, mode_table, modes_in, exp_modals, deep, moved, moments,
    load_sem, send_msg, recv_msg, send_ans, recv_ans, send_mom, recv_mom,
    *, devices, groups,
):
    number = triples_hbm.shape[1]
    needs = 3 * number
    pair_rows = surfaces.shape[0]
    mode_rows = modals_hbm.shape[0]
    modes = pair_slot_hbm.shape[0]
    capacity = needs // devices
    cap = answers.shape[1]
    slots = devices * cap
    bands = -(-mode_rows // 8)
    held_rows = 8 * bands
    spots_all = devices * held_rows
    offset = 2 * KEEP * bands
    width = moved.shape[2]
    everyone = devices * groups
    me = lax.axis_index("dev")
    group = lax.axis_index("grp")
    flat = group * devices + me

    pairs = [
        (triples_hbm, triples), (pair_slot_hbm, pair_slot), (singles_hbm, singles),
        (modals_hbm, modals), (mode_slot_hbm, mode_slot), (small_hbm, small),
        (across_hbm, across), (surfaces, surf),
    ]
    part = energies.shape[1] // CHUNKS
    for i in range(CHUNKS):
        span = pl.ds(i * part, part)
        pairs.append((energies.at[:, span], values.at[:, span]))
    loads = [
        pltpu.make_async_copy(source, target, load_sem.at[min(i, SMALLS + 2)]) for i, (source, target) in enumerate(pairs)
    ]
    for load in loads[: SMALLS + 2]:
        load.start()
    barrier = pltpu.get_barrier_semaphore()

    def after(position, k, size):
        moved_on = position + k
        return jnp.where(moved_on >= size, moved_on - size, moved_on)

    def each_peer(action):
        if devices <= UNROLLED:
            for k in range(1, devices):
                action(after(me, k, devices))
            return

        def step(k, carry):
            action(after(me, k, devices))
            return carry

        lax.fori_loop(1, devices, step, 0)

    def each_other(action):
        each_peer(lambda peer: action(group, peer))
        for k in range(1, groups):
            there = after(group, k, groups)
            action(there, me)
            each_peer(lambda peer: action(there, peer))

    each_other(
        lambda there, peer: pl.semaphore_signal(barrier, inc=1, device_id=(there, peer), device_id_type=MESH)
    )
    for load in loads[SMALLS + 2 :]:
        load.start()
    for load in loads[:SMALLS]:
        load.wait()

    padded[...] = jnp.zeros_like(padded)
    padded[1, 0:modes, 0:modes] = pair_slot[...].astype(f32)
    padded[2, 0:1, 0:modes] = mode_slot[...].astype(f32)
    picks = [triples[p : p + 1, :] for p in range(3)]
    rows = iota((LANES, number), 0)
    on = [rows == pick for pick in picks]
    on_hot = [ones_at(x) for x in on]
    pair_ints = padded[1].astype(jnp.int32)
    first_two = jnp.concatenate(on_hot[:2], axis=1)
    lines = 128.0 * nn((pair_ints >> 7).astype(f32).astype(bf16), first_two)
    lines = lines + nn((pair_ints & 127).astype(f32).astype(bf16), first_two)
    chosen = [
        total(jnp.where(on[1], lines[:, :number], 0.0), 0),
        total(jnp.where(on[2], lines[:, :number], 0.0), 0),
        total(jnp.where(on[2], lines[:, number:], 0.0), 0),
    ]
    flips = [picks[0] > picks[1], picks[0] > picks[2], picks[1] > picks[2]]
    pair_ids = (jnp.concatenate(chosen, axis=1) + 0.5).astype(jnp.int32)
    holders = iota((devices, needs), 0)
    held = (pair_ids >= holders * pair_rows) & (pair_ids < (holders + 1) * pair_rows)
    held_hot = ones_at(held)
    owner = total(jnp.where(held, holders, 0), 0)
    local = pair_ids - owner * pair_rows
    before = ones_at(iota((number, number), 0) < iota((number, number), 1))
    seen = jnp.zeros((devices, 1), f32)
    ranks = []
    for p in range(3):
        block = held_hot[:, p * number : (p + 1) * number]
        mine = held[:, p * number : (p + 1) * number]
        ranks.append(total(jnp.where(mine, nn(block, before) + seen, 0.0), 0))
        seen = seen + total(jnp.where(mine, 1.0, 0.0), 1)
    rank = (jnp.concatenate(ranks, axis=1) + 0.5).astype(jnp.int32)
    place = owner * cap + rank
    at_rank = ones_at(iota((LANES, needs), 0) == rank)
    modes_hot = jnp.concatenate(on_hot, axis=1)
    slot_ids = (nn(padded[2, 0:8, :].astype(bf16), modes_hot)[0:1, :] + 0.5).astype(jnp.int32)
    homes = iota((devices, needs), 0)
    home_row = total(jnp.where(slot_ids >= (homes + 1) * mode_rows, 1, 0), 0)
    at_home = slot_ids - home_row * mode_rows
    home_hot = ones_at(homes == home_row)
    spot = home_row * held_rows + at_home
    spots = [spot[:, p * number : (p + 1) * number] for p in range(3)]
    lower, upper, third = [], [], []
    for p, (one, two, three) in enumerate(((0, 1, 2), (0, 2, 1), (1, 2, 0))):
        lower.append(jnp.where(flips[p], spots[two], spots[one]))
        upper.append(jnp.where(flips[p], spots[one], spots[two]))
        third.append(spots[three])
    told = [local >> 4, local & 15] + [jnp.concatenate(x, axis=1) for x in (lower, upper, third)]
    told = [jnp.where(held, x.astype(f32), 0.0).astype(bf16) for x in told]
    sorted_told = nt(jnp.concatenate(told, axis=0), at_rank)
    parts = [sorted_told[f * devices : (f + 1) * devices, :] for f in range(5)]
    requests = [16.0 * parts[0] + parts[1]] + parts[2:]

    modes_in[...] = jnp.zeros_like(modes_in)
    modes_in[0:mode_rows, 0 : G * S] = modals[...]
    modes_in[0:mode_rows, G * S : G * S + G] = singles[...]
    every = modes_in[:, 0 : G * S]
    spread = small[:, 0 : G * S]
    lane = iota((KEEP, G * S), 1)
    ground_weights = jnp.where((lane & (S - 1)) == 0, spread, 0.0)
    ground_here = nt(every * every, ground_weights, highest)
    single_here = nt(modes_in[:, G * S : G * S + G], small[:, G * S : G * S + G], highest)
    padded[3, 0 : modes_in.shape[0], 0:KEEP] = ground_here
    padded[3, 0 : modes_in.shape[0], KEEP : 2 * KEEP] = single_here
    base = padded[3, 0:8, :]
    for q in range(1, bands):
        base = base + pltpu.roll(padded[3, 8 * q : 8 * q + 8, :], 2 * KEEP * q, 1)
    asked = [pltpu.roll(x, offset, 1) for x in requests]
    blank = jnp.zeros((8 - len(asked), LANES), f32)
    for p in range(devices):
        message[p] = base + jnp.concatenate([x[p : p + 1, :] for x in asked] + [blank], axis=0)
    received[me] = message[me]

    pl.semaphore_wait(barrier, everyone - 1)

    def exchange(source, target, send_sem, recv_sem, there, peer):
        return pltpu.make_async_remote_copy(
            src_ref=source, dst_ref=target, send_sem=send_sem, recv_sem=recv_sem,
            device_id=(there, peer), device_id_type=MESH,
        )

    def message_copy(peer, slot, count=None):
        rows = (lambda i: i) if count is None else (lambda i: pl.ds(0, count))
        return exchange(message.at[rows(peer)], received.at[rows(slot)], send_msg, recv_msg, group, peer)

    def answer_copy(peer, slot, count=None):
        rows = (lambda i: i) if count is None else (lambda i: pl.ds(0, count))
        return exchange(answers.at[rows(peer)], arrived.at[rows(slot)], send_ans, recv_ans, group, peer)

    neighbour = lax.rem(me + 1, devices)
    all_messages = message_copy(neighbour, 0, devices - 1)
    all_answers = answer_copy(neighbour, 0, devices - 1)
    all_moments = exchange(
        moments.at[pl.ds(0, everyone - 1)], moments.at[pl.ds(0, everyone - 1)], send_mom, recv_mom, group, neighbour
    )

    each_peer(lambda peer: message_copy(peer, me).start())

    loads[SMALLS].wait()
    loads[SMALLS + 1].wait()
    table_rows = table.shape[1]
    done = 0
    while done < table_rows:
        size = min(256, table_rows - done)
        have = min(size, pair_rows - done)
        whole = have // 16 * 16
        pieces = []
        if whole:
            pieces.append(surf[done : done + whole, :])
        if size > whole:
            rest = jnp.zeros((size - whole, G * G), f32)
            if have > whole:
                tail = jnp.concatenate(
                    [surf[done + whole : done + have, :], jnp.zeros((16 - (have - whole), G * G), f32)], axis=0
                )
                pieces.append(tail)
                rest = jnp.zeros((size - whole - 16, G * G), f32)
            if rest.shape[0]:
                pieces.append(None)
        at = done
        for piece in pieces:
            if piece is None:
                table[:, at : done + size, :] = jnp.zeros((2, done + size - at, AREA), bf16)
                continue
            high, low = split(piece)
            both_parts = nn(high, across[...])
            fitted = both_parts[:, 0:AREA] + both_parts[:, AREA : 2 * AREA] + nn(low, across[:, 0:AREA])
            count = piece.shape[0]
            part_high, part_low = split(fitted)
            table[0, at : at + count, :] = part_high
            table[1, at : at + count, :] = part_low
            at += count
        done += size

    pltpu.make_async_copy(energies, values, load_sem.at[SMALLS + 2]).wait()

    def inner_fit(step):
        js = members(step)
        for first in range(0, 4, 1):
            points = [g for j in js[first : first + 1] for g in (j, G - 1 - j)]
            rows = jnp.concatenate([values[:, g * G * G : (g + 1) * G * G] for g in points], axis=0)
            both = nn(rows, across[...])
            plane = both[:, 0:AREA] + both[:, AREA : 2 * AREA]
            for i in range(1):
                front = plane[2 * i * number : (2 * i + 1) * number]
                back = plane[(2 * i + 1) * number : (2 * i + 2) * number]
                planes[step % 2, first + i] = (front + back).T
                planes[step % 2, 4 + first + i] = (front - back).T

    def outer_fit(step):
        for block in range(AREA // 8):
            span = slice(block * 8, block * 8 + 8)
            sums = [planes[step % 2, i, span, :] for i in range(4)]
            differences = [planes[step % 2, 4 + i, span, :] for i in range(4)]
            for c, value in enumerate(fit_orders(step, sums, differences)):
                acc[c, span, :] = value if step == 0 else acc[c, span, :] + value

    for step in range(EARLY):
        inner_fit(step)
        if step:
            outer_fit(step - 1)

    all_messages.wait_recv()
    wanted = [received[p, f : f + 1, :] for f in range(4) for p in range(devices)]
    if 4 * devices < LANES:
        wanted.append(jnp.zeros((LANES - 4 * devices, LANES), f32))
    wanted = (jnp.concatenate(wanted, axis=0).T[offset : offset + cap, :] + 0.5).astype(jnp.int32)
    in_table = iota((cap, table_rows), 1)
    if cap > capacity:
        modes_of[...] = jnp.zeros_like(modes_of)
    found = []
    half = max(1, devices // 2)
    for start in range(0, devices, half):
        rows_hot = jnp.concatenate(
            [ones_at(wanted[:, p : p + 1] == in_table) for p in range(start, start + half)], axis=0
        )
        found.append(nn(rows_hot, table[0]) + nn(rows_hot, table[1]))
        answers[start : start + half] = found[-1].reshape(half, cap, AREA)
    found = jnp.concatenate(found, axis=0)
    arrived[me] = answers[me]
    for k in sorted(range(1, devices), key=lambda k: abs(2 * k - devices)):
        answer_copy(after(me, k, devices), me).start()

    sent = received[...].reshape(devices * 8, LANES)
    for q in range(bands):
        turned = pltpu.roll(sent, LANES - 2 * KEEP * q, 1) if q else sent
        mode_table[:, 8 * q : 8 * q + 8, :] = turned.reshape(devices, 8, LANES)
    mode_rows_all = mode_table[...].reshape(spots_all, LANES)[:, 0 : 2 * KEEP]
    tables_high, tables_low = split(mode_rows_all)
    spot_hot = ones_at(iota((spots_all, needs), 0) == spot)
    taken = tn(tables_high, spot_hot) + tn(tables_low, spot_hot)
    ground = [taken[0:KEEP, p * number : (p + 1) * number] for p in range(3)]
    single = [taken[KEEP : 2 * KEEP, p * number : (p + 1) * number] for p in range(3)]

    in_spots = iota((capacity, spots_all), 1)
    for f in range(3):
        for p in range(devices):
            column = wanted[0:capacity, (f + 1) * devices + p : (f + 1) * devices + p + 1]
            hot_row = ones_at(column == in_spots)
            modes_of[f, p, 0:capacity, 0:spots_all] = hot_row
            modes_of[f, p, 0:capacity, spots_all : 2 * spots_all] = hot_row
    columns = iota((KEEP, AREA), 1)
    index = iota((KEEP, AREA), 0)
    by_first = ones_at((columns >> 4) == index)
    by_second = ones_at((columns & (KEEP - 1)) == index)
    by_zero = ones_at(index == 0)
    patterns = jnp.concatenate([by_first, by_second, by_zero], axis=1)
    wide_high, wide_low = split(nn(tables_high[:, 0:KEEP], patterns) + nn(tables_low[:, 0:KEEP], patterns))
    wide_tables = jnp.concatenate([wide_high, wide_low], axis=0)
    def fold_orders(values, pattern):
        high, low = split(values)
        return nt(high, pattern) + nt(low, pattern)

    def fit_step(step):
        if step < STEPS:
            inner_fit(step)
        if step:
            outer_fit(step - 1)

    ground_lower, ground_upper, ground_third = [
        nn(modes_of[f].reshape(slots, 2 * spots_all), wide_tables[:, f * AREA : (f + 1) * AREA]) for f in range(3)
    ]

    fit_step(EARLY)

    seen_upper = found * ground_upper
    takes = [
        fold_orders(seen_upper * ground_third, by_first),
        fold_orders(found * ground_lower * ground_third, by_second),
        fold_orders(seen_upper * ground_lower, by_zero),
    ]
    fit_step(EARLY + 1)

    takes_high, takes_low = split(jnp.concatenate(takes, axis=0))
    asked_spots = []
    for f in range(3):
        for p in range(devices):
            asked_spots.append(received[p, f + 1 : f + 2, offset : offset + cap])
    asked_spots = jnp.concatenate(asked_spots, axis=1)
    spot_rows = (asked_spots + 0.5).astype(jnp.int32)
    turned_hot = ones_at(iota((spots_all, 3 * slots), 0) == spot_rows)
    owed = nn(turned_hot, takes_high) + nn(turned_hot, takes_low)
    owed_high, owed_low = split(owed)
    repeat = ones_at((iota((KEEP, width), 1) & (KEEP - 1)) == iota((KEEP, width), 0))
    owed = nn(owed_high, repeat) + nn(owed_low, repeat)
    wide_row = iota((spots_all, width), 0) & (held_rows - 1)
    owed_high, owed_low = split(jnp.where(wide_row == (iota((spots_all, width), 1) >> 4), owed, 0.0))
    of_home = ones_at((iota((devices, spots_all), 1) // held_rows) == iota((devices, spots_all), 0))
    owed = nn(of_home, owed_high) + nn(of_home, owed_low)
    for step in range(EARLY + 2, STEPS + 1):
        fit_step(step)

    first_row = iota((KEEP, number), 0) == 0
    for c in range(KEEP):
        here = jnp.where(first_row, single[0][c : c + 1, :], 0.0)
        acc[c, 0:KEEP, :] -= here + single[2] if c == 0 else here
    acc[0, pl.ds(0, KEEP, stride=KEEP), :] -= single[1]
    low3, high3 = ground[2][0:8], ground[2][8:16]
    rows1 = [ground[0][c : c + 1, :] for c in range(KEEP)]
    partial1 = [jnp.zeros((8, number), f32) for _ in range(KEEP)]
    field2 = []
    field3 = [jnp.zeros((8, number), f32) for _ in range(2)]
    for d in range(KEEP):
        row2 = ground[1][d : d + 1, :]
        inner = jnp.zeros((8, number), f32)
        for h, part3 in enumerate((low3, high3)):
            weight = row2 * part3
            mixed = jnp.zeros((8, number), f32)
            for c in range(KEEP):
                value = acc[c, d * KEEP + 8 * h : d * KEEP + 8 * h + 8, :]
                partial1[c] = partial1[c] + value * weight
                mixed = mixed + value * rows1[c]
            inner = inner + mixed * part3
            field3[h] = field3[h] + mixed * row2
        field2.append(total(inner, 0))
    field1 = jnp.concatenate([total(x, 0) for x in partial1], axis=0)
    field2 = jnp.concatenate(field2, axis=0)
    field3 = jnp.concatenate(field3, axis=0)
    energy = total(field1 * ground[0], 0)

    fields = jnp.concatenate([field1, field2, field3], axis=1)
    fields = jnp.concatenate([fields] * (width // KEEP), axis=0)
    fields_high, fields_low = split(jnp.where((iota((width, needs), 0) >> 4) == at_home, fields, 0.0))
    sums = nt(home_hot, fields_high) + nt(home_hot, fields_low) - owed
    for p in range(devices):
        moved[p] = sums[p : p + 1, :]
    moments[flat] = moved[me]

    each_other(
        lambda there, peer: exchange(moved.at[peer], moments.at[flat], send_mom, recv_mom, there, peer).start()
    )

    rows16 = modes_in.shape[0]
    for g in range(G):
        exp_modals[g * rows16 : (g + 1) * rows16, 0:S] = modes_in[:, g * S : (g + 1) * S]
    pieces = exp_modals[:, 0:S]
    piece_high, piece_low = split(pieces)
    products = (nn(piece_high, by_first) + nn(piece_low, by_first)) * (nn(piece_high, by_second) + nn(piece_low, by_second))
    products_high, products_low = split(products)
    tall = jnp.concatenate([spread] * (width // KEEP), axis=0)
    own_row = (iota(tall.shape, 1) & (rows16 - 1)) == (iota(tall.shape, 0) >> 4)
    tall_high, tall_low = split(jnp.where(own_row, tall, 0.0))
    deep_high, deep_low = split(
        nn(tall_high, products_high) + nn(tall_high, products_low) + nn(tall_low, products_high)
    )
    deep[0] = deep_high
    deep[1] = deep_low

    all_answers.wait_recv()
    place_hot = ones_at(iota((slots, needs), 0) == place)
    arrived_high, arrived_low = split(arrived[...].reshape(slots, AREA))
    ordered = tn(arrived_high, place_hot) + tn(arrived_low, place_hot)
    for p in range(3):
        pair_t[p] = ordered[:, p * number : (p + 1) * number]

    def pair_rows_of(p, c):
        straight = pair_t[p, c * KEEP : (c + 1) * KEEP, :]
        turned_rows = pair_t[p, pl.ds(c, KEEP, stride=KEEP), :]
        return jnp.where(flips[p], turned_rows, straight)

    for c in range(KEEP):
        acc[c, pl.ds(0, KEEP, stride=KEEP), :] -= pair_rows_of(0, c)
        acc[c, 0:KEEP, :] -= pair_rows_of(1, c)
        acc[0, c * KEEP : (c + 1) * KEEP, :] -= pair_rows_of(2, c)

    for p, (one, two, three) in enumerate(((0, 1, 2), (0, 2, 1), (1, 2, 0))):
        ground_low = jnp.where(flips[p], ground[two], ground[one])
        ground_high = jnp.where(flips[p], ground[one], ground[two])
        share = jnp.zeros((KEEP, number), f32)
        for c in range(KEEP):
            share = share + pair_t[p, c * KEEP : (c + 1) * KEEP, :] * ground_low[c : c + 1, :]
        energy = energy - ground[three][0:1, :] * total(share * ground_high, 0)
    energy_out[...] = energy

    for c in range(KEEP):
        coefficients[:, c * AREA : (c + 1) * AREA] = acc[c].T.astype(bf16)

    all_moments.wait_recv()
    summed = moments[0]
    for k in range(1, everyone):
        summed = summed + moments[k]
    chosen_rows = (iota((rows16, width), 1) >> 4) == iota((rows16, width), 0)
    mean_high, mean_low = split(jnp.where(chosen_rows, summed, 0.0))
    mean = nn(mean_high, deep[0]) + nn(mean_high, deep[1]) + nn(mean_low, deep[0])
    mean_out[...] = mean[0:mode_rows, :]

    all_messages.wait_send()
    all_answers.wait_send()
    all_moments.wait_send()


def write_kernel(coefficients, energy, mean, coefficients_out, energy_out, mean_out, sems):
    copies = [
        pltpu.make_async_copy(source, target, sems.at[i])
        for i, (source, target) in enumerate(
            [(coefficients, coefficients_out), (energy, energy_out), (mean, mean_out)]
        )
    ]
    for copy in copies:
        copy.start()
    for copy in copies:
        copy.wait()


def body(energies, triples, pair_surfaces, pair_slot, single_surfaces, modals, mode_slot):
    devices = lax.axis_size("dev")
    groups = lax.axis_size("grp")
    number = triples.shape[0]
    pair_rows = pair_surfaces.shape[0]
    mode_rows = modals.shape[0]
    cap = round_up(3 * number // devices, 16)
    table_rows = round_up(pair_rows, 256)
    width = round_up(mode_rows * KEEP, LANES)
    rows16 = 16
    held_rows = round_up(mode_rows, 8)
    spots_all = devices * held_rows
    everyone = devices * groups
    vmem = pl.BlockSpec(memory_space=pltpu.VMEM)
    hbm = pl.BlockSpec(memory_space=pltpu.HBM)
    small_shapes = [
        (triples.shape[::-1], jnp.int32), (pair_slot.shape, jnp.int32), (single_surfaces.shape, f32),
        (modals.shape, f32), ((1, mode_slot.shape[0]), jnp.int32), (SMALL.shape, f32),
    ]
    results = [
        jax.ShapeDtypeStruct((number, KEEP * AREA), bf16),
        jax.ShapeDtypeStruct((1, number), f32),
        jax.ShapeDtypeStruct((mode_rows, S * S), f32),
    ]
    in_vmem = pl.pallas_call(
        functools.partial(kernel, devices=devices, groups=groups),
        in_specs=[hbm] * 9,
        out_specs=[vmem, vmem, vmem],
        out_shape=results,
        scratch_shapes=[
            *[pltpu.VMEM(shape, kind) for shape, kind in small_shapes],
            pltpu.VMEM(energies.shape, bf16),
            pltpu.VMEM(pair_surfaces.shape, f32),
            pltpu.VMEM(ACROSS.shape, bf16),
            pltpu.VMEM((2, 8, AREA, number), f32),
            pltpu.VMEM((KEEP, AREA, number), f32),
            pltpu.VMEM((2, table_rows, AREA), bf16),
            pltpu.VMEM((devices, cap, AREA), f32),
            pltpu.VMEM((devices, cap, AREA), f32),
            pltpu.VMEM((3, AREA, number), f32),
            pltpu.VMEM((4, LANES, LANES), f32),
            pltpu.VMEM((devices, 8, LANES), f32),
            pltpu.VMEM((devices, 8, LANES), f32),
            pltpu.VMEM((3, devices, cap, 2 * spots_all), bf16),
            pltpu.VMEM((devices, held_rows, LANES), f32),
            pltpu.VMEM((rows16, SMALL.shape[1]), f32),
            pltpu.VMEM((G * rows16, LANES), f32),
            pltpu.VMEM((2, width, AREA), bf16),
            pltpu.VMEM((devices, 1, width), f32),
            pltpu.VMEM((everyone, 1, width), f32),
            pltpu.SemaphoreType.DMA((SMALLS + 3,)),
            *[pltpu.SemaphoreType.DMA] * 6,
        ],
        compiler_params=pltpu.CompilerParams(
            collective_id=0, has_side_effects=True, vmem_limit_bytes=32 * 1024 * 1024
        ),
    )(
        *[
            pltpu.with_memory_space_constraint(x, pltpu.HBM)
            for x in (
                energies, triples.T, pair_surfaces, pair_slot, single_surfaces, modals, mode_slot.reshape(1, -1),
                jnp.asarray(ACROSS), jnp.asarray(SMALL),
            )
        ]
    )
    coefficients, energy, mean = pl.pallas_call(
        write_kernel,
        in_specs=[vmem] * 3,
        out_specs=[hbm] * 3,
        out_shape=results,
        scratch_shapes=[pltpu.SemaphoreType.DMA((3,))],
        compiler_params=pltpu.CompilerParams(vmem_limit_bytes=1024 * 1024),
    )(*in_vmem)
    return coefficients, energy.reshape(number), mean


def solution(mesh):
    in_specs = (
        P(("grp", "dev"), None),
        P(("grp", "dev"), None),
        P("dev", None),
        P(),
        P("dev", None),
        P("dev", None),
        P(),
    )
    out_specs = (P(("grp", "dev"), None), P(("grp", "dev")), P("dev", None))
    return jax.shard_map(body, mesh=mesh, in_specs=in_specs, out_specs=out_specs, check_vma=False)
```

```python
import functools

import jax
import jax.numpy as jnp
import numpy as np
from jax import lax
from jax.experimental import pallas as pl
from jax.experimental.pallas import tpu as pltpu
from jax.sharding import PartitionSpec as P

G = 32
KEEP = 16
S = 16
AREA = KEEP * KEEP
HALF = G // 2
LANES = 128
STEPS = 4
EARLY = 1
CHUNKS = 8
SMALLS = 6
UNROLLED = 8
MESH = pl.DeviceIdType.MESH
f32 = jnp.float32
bf16 = jnp.bfloat16
highest = lax.Precision.HIGHEST


def np_tables():
    orders = np.arange(KEEP, dtype=np.float64)
    points = np.arange(G, dtype=np.float64) + 0.5
    cosines = np.cos(np.pi * orders[:, None] * points[None, :] / G)
    weights = np.where(orders == 0, 1.0, 2.0) / G
    return cosines, weights[:, None] * cosines


COS, FIT = np_tables()


def split_np(values):
    values = np.asarray(values, np.float32)
    high = values.astype(jnp.bfloat16)
    return high, (values - high.astype(np.float32)).astype(jnp.bfloat16)


INNER = np.einsum("dh,el->hlde", FIT, FIT).reshape(G * G, AREA)
ACROSS = np.concatenate(split_np(INNER), axis=1)
SMALL = np.concatenate([np.repeat(COS, S, axis=1), FIT, np.zeros((KEEP, LANES - G))], axis=1).astype(np.float32)


def round_up(value, step):
    return -(-value // step) * step


def iota(shape, axis):
    return lax.broadcasted_iota(jnp.int32, shape, axis)


def nn(a, b, precision=None):
    return lax.dot_general(a, b, (((1,), (0,)), ((), ())), precision=precision, preferred_element_type=f32)


def nt(a, b, precision=None):
    return lax.dot_general(a, b, (((1,), (1,)), ((), ())), precision=precision, preferred_element_type=f32)


def tn(a, b, precision=None):
    return lax.dot_general(a, b, (((0,), (0,)), ((), ())), precision=precision, preferred_element_type=f32)


def split(values):
    high = values.astype(bf16)
    return high, (values - high.astype(f32)).astype(bf16)


def ones_at(mask):
    return jnp.where(mask, 1.0, 0.0).astype(bf16)


def total(values, axis):
    return jnp.sum(values, axis=axis, keepdims=True)


def members(step):
    return step, 15 - step, 7 - step, 8 + step


def fit_orders(step, s, d):
    js = members(step)
    u, v = (s[0] + s[1], s[2] + s[3]), (s[0] - s[1], s[2] - s[3])
    out = []
    for c in range(KEEP):
        if c % 2:
            terms = list(zip(js, d))
        elif c % 4:
            terms = [(js[0], v[0]), (js[2], v[1])]
        elif c % 8:
            terms = [(js[0], u[0] - u[1])]
        else:
            terms = [(js[0], u[0] + u[1])]
        value = None
        for j, term in terms:
            scaled = float(FIT[c, j]) * term
            value = scaled if value is None else value + scaled
        out.append(value)
    return out


def kernel(
    energies, triples_hbm, surfaces, pair_slot_hbm, singles_hbm, modals_hbm, mode_slot_hbm, across_hbm, small_hbm,
    coefficients, energy_out, mean_out,
    triples, pair_slot, singles, modals, mode_slot, small,
    values, surf, across, planes, acc, table, answers, arrived, pair_t, padded, message, received,
    modes_of, mode_table, modes_in, exp_modals, deep, moved, moments,
    load_sem, send_msg, recv_msg, send_ans, recv_ans, send_mom, recv_mom,
    *, devices, groups,
):
    number = triples_hbm.shape[1]
    needs = 3 * number
    pair_rows = surfaces.shape[0]
    mode_rows = modals_hbm.shape[0]
    modes = pair_slot_hbm.shape[0]
    capacity = needs // devices
    cap = answers.shape[1]
    slots = devices * cap
    bands = -(-mode_rows // 8)
    held_rows = 8 * bands
    spots_all = devices * held_rows
    offset = 2 * KEEP * bands
    width = moved.shape[2]
    everyone = devices * groups
    me = lax.axis_index("dev")
    group = lax.axis_index("grp")
    flat = group * devices + me

    pairs = [
        (triples_hbm, triples), (pair_slot_hbm, pair_slot), (singles_hbm, singles),
        (modals_hbm, modals), (mode_slot_hbm, mode_slot), (small_hbm, small),
        (across_hbm, across), (surfaces, surf),
    ]
    part = energies.shape[1] // CHUNKS
    for i in range(CHUNKS):
        span = pl.ds(i * part, part)
        pairs.append((energies.at[:, span], values.at[:, span]))
    loads = [
        pltpu.make_async_copy(source, target, load_sem.at[min(i, SMALLS + 2)]) for i, (source, target) in enumerate(pairs)
    ]
    for load in loads[: SMALLS + 2]:
        load.start()
    barrier = pltpu.get_barrier_semaphore()

    def after(position, k, size):
        moved_on = position + k
        return jnp.where(moved_on >= size, moved_on - size, moved_on)

    def each_peer(action):
        if devices <= UNROLLED:
            for k in range(1, devices):
                action(after(me, k, devices))
            return

        def step(k, carry):
            action(after(me, k, devices))
            return carry

        lax.fori_loop(1, devices, step, 0)

    def each_other(action):
        each_peer(lambda peer: action(group, peer))
        for k in range(1, groups):
            there = after(group, k, groups)
            action(there, me)
            each_peer(lambda peer: action(there, peer))

    each_other(
        lambda there, peer: pl.semaphore_signal(barrier, inc=1, device_id=(there, peer), device_id_type=MESH)
    )
    for load in loads[SMALLS + 2 :]:
        load.start()
    for load in loads[:SMALLS]:
        load.wait()

    padded[...] = jnp.zeros_like(padded)
    padded[1, 0:modes, 0:modes] = pair_slot[...].astype(f32)
    padded[2, 0:1, 0:modes] = mode_slot[...].astype(f32)
    picks = [triples[p : p + 1, :] for p in range(3)]
    rows = iota((LANES, number), 0)
    on = [rows == pick for pick in picks]
    on_hot = [ones_at(x) for x in on]
    pair_ints = padded[1].astype(jnp.int32)
    first_two = jnp.concatenate(on_hot[:2], axis=1)
    lines = 128.0 * nn((pair_ints >> 7).astype(f32).astype(bf16), first_two)
    lines = lines + nn((pair_ints & 127).astype(f32).astype(bf16), first_two)
    chosen = [
        total(jnp.where(on[1], lines[:, :number], 0.0), 0),
        total(jnp.where(on[2], lines[:, :number], 0.0), 0),
        total(jnp.where(on[2], lines[:, number:], 0.0), 0),
    ]
    flips = [picks[0] > picks[1], picks[0] > picks[2], picks[1] > picks[2]]
    pair_ids = (jnp.concatenate(chosen, axis=1) + 0.5).astype(jnp.int32)
    holders = iota((devices, needs), 0)
    held = (pair_ids >= holders * pair_rows) & (pair_ids < (holders + 1) * pair_rows)
    held_hot = ones_at(held)
    owner = total(jnp.where(held, holders, 0), 0)
    local = pair_ids - owner * pair_rows
    before = ones_at(iota((number, number), 0) < iota((number, number), 1))
    seen = jnp.zeros((devices, 1), f32)
    ranks = []
    for p in range(3):
        block = held_hot[:, p * number : (p + 1) * number]
        mine = held[:, p * number : (p + 1) * number]
        ranks.append(total(jnp.where(mine, nn(block, before) + seen, 0.0), 0))
        seen = seen + total(jnp.where(mine, 1.0, 0.0), 1)
    rank = (jnp.concatenate(ranks, axis=1) + 0.5).astype(jnp.int32)
    place = owner * cap + rank
    at_rank = ones_at(iota((LANES, needs), 0) == rank)
    modes_hot = jnp.concatenate(on_hot, axis=1)
    slot_ids = (nn(padded[2, 0:8, :].astype(bf16), modes_hot)[0:1, :] + 0.5).astype(jnp.int32)
    homes = iota((devices, needs), 0)
    home_row = total(jnp.where(slot_ids >= (homes + 1) * mode_rows, 1, 0), 0)
    at_home = slot_ids - home_row * mode_rows
    home_hot = ones_at(homes == home_row)
    spot = home_row * held_rows + at_home
    spots = [spot[:, p * number : (p + 1) * number] for p in range(3)]
    lower, upper, third = [], [], []
    for p, (one, two, three) in enumerate(((0, 1, 2), (0, 2, 1), (1, 2, 0))):
        lower.append(jnp.where(flips[p], spots[two], spots[one]))
        upper.append(jnp.where(flips[p], spots[one], spots[two]))
        third.append(spots[three])
    told = [local >> 4, local & 15] + [jnp.concatenate(x, axis=1) for x in (lower, upper, third)]
    told = [jnp.where(held, x.astype(f32), 0.0).astype(bf16) for x in told]
    sorted_told = nt(jnp.concatenate(told, axis=0), at_rank)
    parts = [sorted_told[f * devices : (f + 1) * devices, :] for f in range(5)]
    requests = [16.0 * parts[0] + parts[1]] + parts[2:]

    modes_in[...] = jnp.zeros_like(modes_in)
    modes_in[0:mode_rows, 0 : G * S] = modals[...]
    modes_in[0:mode_rows, G * S : G * S + G] = singles[...]
    every = modes_in[:, 0 : G * S]
    spread = small[:, 0 : G * S]
    lane = iota((KEEP, G * S), 1)
    ground_weights = jnp.where((lane & (S - 1)) == 0, spread, 0.0)
    ground_here = nt(every * every, ground_weights, highest)
    single_here = nt(modes_in[:, G * S : G * S + G], small[:, G * S : G * S + G], highest)
    padded[3, 0 : modes_in.shape[0], 0:KEEP] = ground_here
    padded[3, 0 : modes_in.shape[0], KEEP : 2 * KEEP] = single_here
    base = padded[3, 0:8, :]
    for q in range(1, bands):
        base = base + pltpu.roll(padded[3, 8 * q : 8 * q + 8, :], 2 * KEEP * q, 1)
    asked = [pltpu.roll(x, offset, 1) for x in requests]
    blank = jnp.zeros((8 - len(asked), LANES), f32)
    for p in range(devices):
        message[p] = base + jnp.concatenate([x[p : p + 1, :] for x in asked] + [blank], axis=0)
    received[me] = message[me]

    pl.semaphore_wait(barrier, everyone - 1)

    def exchange(source, target, send_sem, recv_sem, there, peer):
        return pltpu.make_async_remote_copy(
            src_ref=source, dst_ref=target, send_sem=send_sem, recv_sem=recv_sem,
            device_id=(there, peer), device_id_type=MESH,
        )

    def message_copy(peer, slot, count=None):
        rows = (lambda i: i) if count is None else (lambda i: pl.ds(0, count))
        return exchange(message.at[rows(peer)], received.at[rows(slot)], send_msg, recv_msg, group, peer)

    def answer_copy(peer, slot, count=None):
        rows = (lambda i: i) if count is None else (lambda i: pl.ds(0, count))
        return exchange(answers.at[rows(peer)], arrived.at[rows(slot)], send_ans, recv_ans, group, peer)

    neighbour = lax.rem(me + 1, devices)
    all_messages = message_copy(neighbour, 0, devices - 1)
    all_answers = answer_copy(neighbour, 0, devices - 1)
    all_moments = exchange(
        moments.at[pl.ds(0, everyone - 1)], moments.at[pl.ds(0, everyone - 1)], send_mom, recv_mom, group, neighbour
    )

    each_peer(lambda peer: message_copy(peer, me).start())

    loads[SMALLS].wait()
    loads[SMALLS + 1].wait()
    table_rows = table.shape[1]
    done = 0
    while done < table_rows:
        size = min(256, table_rows - done)
        have = min(size, pair_rows - done)
        whole = have // 16 * 16
        pieces = []
        if whole:
            pieces.append(surf[done : done + whole, :])
        if size > whole:
            rest = jnp.zeros((size - whole, G * G), f32)
            if have > whole:
                tail = jnp.concatenate(
                    [surf[done + whole : done + have, :], jnp.zeros((16 - (have - whole), G * G), f32)], axis=0
                )
                pieces.append(tail)
                rest = jnp.zeros((size - whole - 16, G * G), f32)
            if rest.shape[0]:
                pieces.append(None)
        at = done
        for piece in pieces:
            if piece is None:
                table[:, at : done + size, :] = jnp.zeros((2, done + size - at, AREA), bf16)
                continue
            high, low = split(piece)
            both_parts = nn(high, across[...])
            fitted = both_parts[:, 0:AREA] + both_parts[:, AREA : 2 * AREA] + nn(low, across[:, 0:AREA])
            count = piece.shape[0]
            part_high, part_low = split(fitted)
            table[0, at : at + count, :] = part_high
            table[1, at : at + count, :] = part_low
            at += count
        done += size

    pltpu.make_async_copy(energies, values, load_sem.at[SMALLS + 2]).wait()

    def inner_fit(step):
        js = members(step)
        for first in range(0, 4, 1):
            points = [g for j in js[first : first + 1] for g in (j, G - 1 - j)]
            rows = jnp.concatenate([values[:, g * G * G : (g + 1) * G * G] for g in points], axis=0)
            both = nn(rows, across[...])
            plane = both[:, 0:AREA] + both[:, AREA : 2 * AREA]
            for i in range(1):
                front = plane[2 * i * number : (2 * i + 1) * number]
                back = plane[(2 * i + 1) * number : (2 * i + 2) * number]
                planes[step % 2, first + i] = (front + back).T
                planes[step % 2, 4 + first + i] = (front - back).T

    def outer_fit(step):
        for block in range(AREA // 8):
            span = slice(block * 8, block * 8 + 8)
            sums = [planes[step % 2, i, span, :] for i in range(4)]
            differences = [planes[step % 2, 4 + i, span, :] for i in range(4)]
            for c, value in enumerate(fit_orders(step, sums, differences)):
                acc[c, span, :] = value if step == 0 else acc[c, span, :] + value

    for step in range(EARLY):
        inner_fit(step)
        if step:
            outer_fit(step - 1)

    all_messages.wait_recv()
    wanted = [received[p, f : f + 1, :] for f in range(4) for p in range(devices)]
    if 4 * devices < LANES:
        wanted.append(jnp.zeros((LANES - 4 * devices, LANES), f32))
    wanted = (jnp.concatenate(wanted, axis=0).T[offset : offset + cap, :] + 0.5).astype(jnp.int32)
    in_table = iota((cap, table_rows), 1)
    if cap > capacity:
        modes_of[...] = jnp.zeros_like(modes_of)
    found = []
    half = max(1, devices // 2)
    for start in range(0, devices, half):
        rows_hot = jnp.concatenate(
            [ones_at(wanted[:, p : p + 1] == in_table) for p in range(start, start + half)], axis=0
        )
        found.append(nn(rows_hot, table[0]) + nn(rows_hot, table[1]))
        answers[start : start + half] = found[-1].reshape(half, cap, AREA)
    found = jnp.concatenate(found, axis=0)
    arrived[me] = answers[me]
    for k in sorted(range(1, devices), key=lambda k: abs(2 * k - devices)):
        answer_copy(after(me, k, devices), me).start()

    sent = received[...].reshape(devices * 8, LANES)
    for q in range(bands):
        turned = pltpu.roll(sent, LANES - 2 * KEEP * q, 1) if q else sent
        mode_table[:, 8 * q : 8 * q + 8, :] = turned.reshape(devices, 8, LANES)
    mode_rows_all = mode_table[...].reshape(spots_all, LANES)[:, 0 : 2 * KEEP]
    tables_high, tables_low = split(mode_rows_all)
    spot_hot = ones_at(iota((spots_all, needs), 0) == spot)
    taken = tn(tables_high, spot_hot) + tn(tables_low, spot_hot)
    ground = [taken[0:KEEP, p * number : (p + 1) * number] for p in range(3)]
    single = [taken[KEEP : 2 * KEEP, p * number : (p + 1) * number] for p in range(3)]

    in_spots = iota((capacity, spots_all), 1)
    for f in range(3):
        for p in range(devices):
            column = wanted[0:capacity, (f + 1) * devices + p : (f + 1) * devices + p + 1]
            hot_row = ones_at(column == in_spots)
            modes_of[f, p, 0:capacity, 0:spots_all] = hot_row
            modes_of[f, p, 0:capacity, spots_all : 2 * spots_all] = hot_row
    columns = iota((KEEP, AREA), 1)
    index = iota((KEEP, AREA), 0)
    by_first = ones_at((columns >> 4) == index)
    by_second = ones_at((columns & (KEEP - 1)) == index)
    by_zero = ones_at(index == 0)
    patterns = jnp.concatenate([by_first, by_second, by_zero], axis=1)
    wide_high, wide_low = split(nn(tables_high[:, 0:KEEP], patterns) + nn(tables_low[:, 0:KEEP], patterns))
    wide_tables = jnp.concatenate([wide_high, wide_low], axis=0)
    def fold_orders(values, pattern):
        high, low = split(values)
        return nt(high, pattern) + nt(low, pattern)

    def fit_step(step):
        if step < STEPS:
            inner_fit(step)
        if step:
            outer_fit(step - 1)

    ground_lower, ground_upper, ground_third = [
        nn(modes_of[f].reshape(slots, 2 * spots_all), wide_tables[:, f * AREA : (f + 1) * AREA]) for f in range(3)
    ]

    fit_step(EARLY)

    seen_upper = found * ground_upper
    takes = [
        fold_orders(seen_upper * ground_third, by_first),
        fold_orders(found * ground_lower * ground_third, by_second),
        fold_orders(seen_upper * ground_lower, by_zero),
    ]
    fit_step(EARLY + 1)

    takes_high, takes_low = split(jnp.concatenate(takes, axis=0))
    asked_spots = []
    for f in range(3):
        for p in range(devices):
            asked_spots.append(received[p, f + 1 : f + 2, offset : offset + cap])
    asked_spots = jnp.concatenate(asked_spots, axis=1)
    spot_rows = (asked_spots + 0.5).astype(jnp.int32)
    turned_hot = ones_at(iota((spots_all, 3 * slots), 0) == spot_rows)
    owed = nn(turned_hot, takes_high) + nn(turned_hot, takes_low)
    owed_high, owed_low = split(owed)
    repeat = ones_at((iota((KEEP, width), 1) & (KEEP - 1)) == iota((KEEP, width), 0))
    owed = nn(owed_high, repeat) + nn(owed_low, repeat)
    wide_row = iota((spots_all, width), 0) & (held_rows - 1)
    owed_high, owed_low = split(jnp.where(wide_row == (iota((spots_all, width), 1) >> 4), owed, 0.0))
    of_home = ones_at((iota((devices, spots_all), 1) // held_rows) == iota((devices, spots_all), 0))
    owed = nn(of_home, owed_high) + nn(of_home, owed_low)
    for step in range(EARLY + 2, STEPS + 1):
        fit_step(step)

    first_row = iota((KEEP, number), 0) == 0
    for c in range(KEEP):
        here = jnp.where(first_row, single[0][c : c + 1, :], 0.0)
        acc[c, 0:KEEP, :] -= here + single[2] if c == 0 else here
    acc[0, pl.ds(0, KEEP, stride=KEEP), :] -= single[1]
    low3, high3 = ground[2][0:8], ground[2][8:16]
    rows1 = [ground[0][c : c + 1, :] for c in range(KEEP)]
    partial1 = [jnp.zeros((8, number), f32) for _ in range(KEEP)]
    field2 = []
    field3 = [jnp.zeros((8, number), f32) for _ in range(2)]
    for d in range(KEEP):
        row2 = ground[1][d : d + 1, :]
        inner = jnp.zeros((8, number), f32)
        for h, part3 in enumerate((low3, high3)):
            weight = row2 * part3
            mixed = jnp.zeros((8, number), f32)
            for c in range(KEEP):
                value = acc[c, d * KEEP + 8 * h : d * KEEP + 8 * h + 8, :]
                partial1[c] = partial1[c] + value * weight
                mixed = mixed + value * rows1[c]
            inner = inner + mixed * part3
            field3[h] = field3[h] + mixed * row2
        field2.append(total(inner, 0))
    field1 = jnp.concatenate([total(x, 0) for x in partial1], axis=0)
    field2 = jnp.concatenate(field2, axis=0)
    field3 = jnp.concatenate(field3, axis=0)
    energy = total(field1 * ground[0], 0)

    fields = jnp.concatenate([field1, field2, field3], axis=1)
    fields = jnp.concatenate([fields] * (width // KEEP), axis=0)
    fields_high, fields_low = split(jnp.where((iota((width, needs), 0) >> 4) == at_home, fields, 0.0))
    sums = nt(home_hot, fields_high) + nt(home_hot, fields_low) - owed
    for p in range(devices):
        moved[p] = sums[p : p + 1, :]
    moments[flat] = moved[me]

    each_other(
        lambda there, peer: exchange(moved.at[peer], moments.at[flat], send_mom, recv_mom, there, peer).start()
    )

    rows16 = modes_in.shape[0]
    for g in range(G):
        exp_modals[g * rows16 : (g + 1) * rows16, 0:S] = modes_in[:, g * S : (g + 1) * S]
    pieces = exp_modals[:, 0:S]
    piece_high, piece_low = split(pieces)
    products = (nn(piece_high, by_first) + nn(piece_low, by_first)) * (nn(piece_high, by_second) + nn(piece_low, by_second))
    products_high, products_low = split(products)
    tall = jnp.concatenate([spread] * (width // KEEP), axis=0)
    own_row = (iota(tall.shape, 1) & (rows16 - 1)) == (iota(tall.shape, 0) >> 4)
    tall_high, tall_low = split(jnp.where(own_row, tall, 0.0))
    deep_high, deep_low = split(
        nn(tall_high, products_high) + nn(tall_high, products_low) + nn(tall_low, products_high)
    )
    deep[0] = deep_high
    deep[1] = deep_low

    all_answers.wait_recv()
    place_hot = ones_at(iota((slots, needs), 0) == place)
    arrived_high, arrived_low = split(arrived[...].reshape(slots, AREA))
    ordered = tn(arrived_high, place_hot) + tn(arrived_low, place_hot)
    for p in range(3):
        pair_t[p] = ordered[:, p * number : (p + 1) * number]

    def pair_rows_of(p, c):
        straight = pair_t[p, c * KEEP : (c + 1) * KEEP, :]
        turned_rows = pair_t[p, pl.ds(c, KEEP, stride=KEEP), :]
        return jnp.where(flips[p], turned_rows, straight)

    for c in range(KEEP):
        acc[c, pl.ds(0, KEEP, stride=KEEP), :] -= pair_rows_of(0, c)
        acc[c, 0:KEEP, :] -= pair_rows_of(1, c)
        acc[0, c * KEEP : (c + 1) * KEEP, :] -= pair_rows_of(2, c)

    for p, (one, two, three) in enumerate(((0, 1, 2), (0, 2, 1), (1, 2, 0))):
        ground_low = jnp.where(flips[p], ground[two], ground[one])
        ground_high = jnp.where(flips[p], ground[one], ground[two])
        share = jnp.zeros((KEEP, number), f32)
        for c in range(KEEP):
            share = share + pair_t[p, c * KEEP : (c + 1) * KEEP, :] * ground_low[c : c + 1, :]
        energy = energy - ground[three][0:1, :] * total(share * ground_high, 0)
    energy_out[...] = energy

    for c in range(KEEP):
        coefficients[:, c * AREA : (c + 1) * AREA] = acc[c].T.astype(bf16)

    all_messages.wait_send()
    all_answers.wait_send()
    all_moments.wait_recv()
    terms = [moments[k] for k in range(everyone)]
    while len(terms) > 1:
        terms = [sum(terms[i + 1 : i + 2], terms[i]) for i in range(0, len(terms), 2)]
    summed = terms[0]
    chosen_rows = (iota((rows16, width), 1) >> 4) == iota((rows16, width), 0)
    mean_high, mean_low = split(jnp.where(chosen_rows, summed, 0.0))
    mean = nn(mean_high, deep[0]) + nn(mean_high, deep[1]) + nn(mean_low, deep[0])
    mean_out[...] = mean[0:mode_rows, :]

    all_moments.wait_send()


def write_kernel(coefficients, energy, mean, coefficients_out, energy_out, mean_out, sems):
    copies = [
        pltpu.make_async_copy(source, target, sems.at[i])
        for i, (source, target) in enumerate(
            [(coefficients, coefficients_out), (energy, energy_out), (mean, mean_out)]
        )
    ]
    for copy in copies:
        copy.start()
    for copy in copies:
        copy.wait()


def body(energies, triples, pair_surfaces, pair_slot, single_surfaces, modals, mode_slot):
    devices = lax.axis_size("dev")
    groups = lax.axis_size("grp")
    number = triples.shape[0]
    pair_rows = pair_surfaces.shape[0]
    mode_rows = modals.shape[0]
    cap = round_up(3 * number // devices, 16)
    table_rows = round_up(pair_rows, 256)
    width = round_up(mode_rows * KEEP, LANES)
    rows16 = 16
    held_rows = round_up(mode_rows, 8)
    spots_all = devices * held_rows
    everyone = devices * groups
    vmem = pl.BlockSpec(memory_space=pltpu.VMEM)
    hbm = pl.BlockSpec(memory_space=pltpu.HBM)
    small_shapes = [
        (triples.shape[::-1], jnp.int32), (pair_slot.shape, jnp.int32), (single_surfaces.shape, f32),
        (modals.shape, f32), ((1, mode_slot.shape[0]), jnp.int32), (SMALL.shape, f32),
    ]
    results = [
        jax.ShapeDtypeStruct((number, KEEP * AREA), bf16),
        jax.ShapeDtypeStruct((1, number), f32),
        jax.ShapeDtypeStruct((mode_rows, S * S), f32),
    ]
    in_vmem = pl.pallas_call(
        functools.partial(kernel, devices=devices, groups=groups),
        in_specs=[hbm] * 9,
        out_specs=[vmem, vmem, vmem],
        out_shape=results,
        scratch_shapes=[
            *[pltpu.VMEM(shape, kind) for shape, kind in small_shapes],
            pltpu.VMEM(energies.shape, bf16),
            pltpu.VMEM(pair_surfaces.shape, f32),
            pltpu.VMEM(ACROSS.shape, bf16),
            pltpu.VMEM((2, 8, AREA, number), f32),
            pltpu.VMEM((KEEP, AREA, number), f32),
            pltpu.VMEM((2, table_rows, AREA), bf16),
            pltpu.VMEM((devices, cap, AREA), f32),
            pltpu.VMEM((devices, cap, AREA), f32),
            pltpu.VMEM((3, AREA, number), f32),
            pltpu.VMEM((4, LANES, LANES), f32),
            pltpu.VMEM((devices, 8, LANES), f32),
            pltpu.VMEM((devices, 8, LANES), f32),
            pltpu.VMEM((3, devices, cap, 2 * spots_all), bf16),
            pltpu.VMEM((devices, held_rows, LANES), f32),
            pltpu.VMEM((rows16, SMALL.shape[1]), f32),
            pltpu.VMEM((G * rows16, LANES), f32),
            pltpu.VMEM((2, width, AREA), bf16),
            pltpu.VMEM((devices, 1, width), f32),
            pltpu.VMEM((everyone, 1, width), f32),
            pltpu.SemaphoreType.DMA((SMALLS + 3,)),
            *[pltpu.SemaphoreType.DMA] * 6,
        ],
        compiler_params=pltpu.CompilerParams(
            collective_id=0, has_side_effects=True, vmem_limit_bytes=32 * 1024 * 1024
        ),
    )(
        *[
            pltpu.with_memory_space_constraint(x, pltpu.HBM)
            for x in (
                energies, triples.T, pair_surfaces, pair_slot, single_surfaces, modals, mode_slot.reshape(1, -1),
                jnp.asarray(ACROSS), jnp.asarray(SMALL),
            )
        ]
    )
    coefficients, energy, mean = pl.pallas_call(
        write_kernel,
        in_specs=[vmem] * 3,
        out_specs=[hbm] * 3,
        out_shape=results,
        scratch_shapes=[pltpu.SemaphoreType.DMA((3,))],
        compiler_params=pltpu.CompilerParams(vmem_limit_bytes=1024 * 1024),
    )(*in_vmem)
    return coefficients, energy.reshape(number), mean


def solution(mesh):
    in_specs = (
        P(("grp", "dev"), None),
        P(("grp", "dev"), None),
        P("dev", None),
        P(),
        P("dev", None),
        P("dev", None),
        P(),
    )
    out_specs = (P(("grp", "dev"), None), P(("grp", "dev")), P("dev", None))
    return jax.shard_map(body, mesh=mesh, in_specs=in_specs, out_specs=out_specs, check_vma=False)
```
